256 devices in a mesh: gx: 8 (over y_hi, x), gy: 8 (over z), gz: 4 (over y_lo, core).
Axes of the slice: x: 4, y: 4 (y_hi: 2, y_lo: 2; y = y_hi * 2 + y_lo), z: 8, core: 2. Of those that a mesh axis runs over, the one named last changes fastest.
Arguments:
- volume: float32 [16, 32, 128, 512], P(None, 'gx', 'gy', 'gz'), may hold values from -26 to 26
- weight: float32 [16, 16, 3, 3, 3], replicated, may hold values from -0.3125 to 0.3125
- gamma: float32 [16], replicated, may hold values from 0.5 to 1.5
- beta: float32 [16], replicated, may hold values from -0.5 to 0.5
- cotangent: float32 [16, 32, 128, 512], P(None, 'gx', 'gy', 'gz'), may hold values from -6 to 6
Outputs:
- input_grad: float32 [16, 32, 128, 512], P(None, 'gx', 'gy', 'gz')
- weight_grad: float32 [16, 16, 3, 3, 3], replicated
- gamma_grad: float32 [16], replicated
- beta_grad: float32 [16], replicated
The draws below stay inside these ranges and needn't reach their ends.
All inputs are finite; a program needn't handle non-finite values.
Results may differ from the reference program's by a relative error of at most 0.0003.
Values sent between devices are 32-bit elements; how exact they have to be, the bound alone decides.
A program may use at most 64 MiB of HBM per device.

```python
import jax
import jax.numpy as jnp
from jax import lax

C = 16
NX = 32
NY = 128
NZ = 512


def draw_volume(key, part):
    first, second, third = jax.random.split(jax.random.fold_in(key, 11), 3)
    channel_scale = jax.random.uniform(second, (C, 1, 1, 1), jnp.float32, 0.5, 2.0)
    offset = jax.random.uniform(third, (C, 1, 1, 1), jnp.float32, -1.0, 1.0)
    ramp = jnp.arange(NX, dtype=jnp.float32) / max(NX - 1, 1)
    rising = jnp.power(3.0, ramp).reshape(1, NX, 1, 1)
    noise = jnp.clip(jax.random.normal(first, (C, NX, NY, NZ), jnp.float32), -4.0, 4.0)
    return channel_scale * rising * noise + offset


def draw_cotangent(key, part):
    first, second, third = jax.random.split(jax.random.fold_in(key, 23), 3)
    ramp = jnp.arange(NX, dtype=jnp.float32) / max(NX - 1, 1)
    tilt = (0.5 + ramp).reshape(1, NX, 1, 1)
    signs = jnp.where(jax.random.uniform(third, (C, 1, 1, 1), jnp.float32) < 0.5, -1.0, 1.0)
    magnitude = jax.random.uniform(second, (C, 1, 1, 1), jnp.float32, 0.4, 1.0)
    noise = jnp.clip(jax.random.normal(first, (C, NX, NY, NZ), jnp.float32), -4.0, 4.0)
    return noise + signs * magnitude * tilt


def gaussian(own_key, dims, deviation, most, kind=jnp.bfloat16):
    drawn = deviation * jax.random.normal(own_key, dims, jnp.float32)
    return jnp.clip(drawn, min=-most, max=most).astype(kind)


def setup_inputs(seed: int = 0) -> dict:
    key_list = jax.random.split(jax.random.key(seed), 6)
    volume = draw_volume(jax.random.fold_in(key_list[5], 71), 0)
    weight = gaussian(key_list[1], (C, C, 3, 3, 3), (C * 27) ** -0.5, 0.3125, jnp.float32)
    gamma = jnp.clip(jax.random.uniform(key_list[2], (C,), jnp.float32, 0.5, 1.5), 0.5, 1.5)
    beta = jnp.clip(jax.random.uniform(key_list[3], (C,), jnp.float32, -0.5, 0.5), -0.5, 0.5)
    cotangent = draw_cotangent(jax.random.fold_in(key_list[5], 71), 0)
    return {"volume": volume, "weight": weight, "gamma": gamma, "beta": beta, "cotangent": cotangent}


def mix(kernel, slab):
    return jnp.einsum('oi,ixyz->oxyz', kernel, slab, precision=lax.Precision.HIGHEST)

def reference(volume, weight, gamma, beta, cotangent):
    count = float(NX * NY * NZ)
    conv = jnp.zeros(volume.shape, jnp.float32)
    for a in range(3):
        for b in range(3):
            for c in range(3):
                conv = conv + mix(weight[:, :, a, b, c], jnp.roll(volume, (1 - a, 1 - b, 1 - c), axis=(1, 2, 3)))
    mean = lax.optimization_barrier(jnp.sum(conv, axis=(1, 2, 3))) / count
    centred = conv - mean[:, None, None, None]
    var = lax.optimization_barrier(jnp.sum(centred * centred, axis=(1, 2, 3))) / count
    rstd = lax.rsqrt(var + 1e-05)
    normed = centred * rstd[:, None, None, None]
    act = gamma[:, None, None, None] * normed + beta[:, None, None, None]
    sig = jax.nn.sigmoid(act)
    act_grad = cotangent * sig * (1.0 + act * (1.0 - sig))
    gamma_grad = lax.optimization_barrier(jnp.sum(act_grad * normed, axis=(1, 2, 3)))
    beta_grad = lax.optimization_barrier(jnp.sum(act_grad, axis=(1, 2, 3)))
    scale = (gamma * rstd)[:, None, None, None]
    conv_grad = scale * (act_grad - (beta_grad / count)[:, None, None, None] - normed * (gamma_grad / count)[:, None, None, None])
    pieces = []
    input_grad = jnp.zeros(volume.shape, jnp.float32)
    for a in range(3):
        for b in range(3):
            for c in range(3):
                slab = jnp.roll(volume, (1 - a, 1 - b, 1 - c), axis=(1, 2, 3))
                pieces.append(jnp.einsum('oxyz,ixyz->oi', conv_grad, slab, precision=lax.Precision.HIGHEST))
                input_grad = input_grad + mix(weight[:, :, a, b, c].T, jnp.roll(conv_grad, (a - 1, b - 1, c - 1), axis=(1, 2, 3)))
    weight_grad = jnp.stack(pieces, axis=2).reshape(C, C, 3, 3, 3)
    return (input_grad, weight_grad, gamma_grad, beta_grad)
```

```python
import functools

import jax
import jax.numpy as jnp
from jax import lax
from jax.experimental import pallas as pl
from jax.experimental.pallas import tpu as pltpu
from jax.sharding import PartitionSpec as P

MESH = pl.DeviceIdType.MESH
L = 128
C = 16
ROWS = 9 * C
BF = jnp.bfloat16
F32 = jnp.float32
SIDES = [(sx, sy) for sx in (-1, 0, 1) for sy in (-1, 0, 1) if (sx, sy) != (0, 0)]


def split(v):
    hi = v.astype(BF)
    lo = (v - hi.astype(F32)).astype(BF)
    return hi, lo


def kernel(
    dims, count, vol_ref, cot_ref, mf_ref, mb_ref, gain_ref, shift_ref,
    out_ref, aux_ref,
    vin, cin, ev, ec, eo, ea, hv, hc, ho, ha, cbv, cbc, cbo,
    r_ref, o_ref, agp, cvp, acc_ref, gw,
    s1x, s1y, s1z, s2x, s2y, s2z, gx_buf, gy_buf, gz_buf, gf_buf,
    in_sem, hsend, hrecv, asend, arecv, gsend, grecv,
):
    nx, ny, nz, X, Y = dims
    W = (Y + 2) * L
    I0, I1 = L, (Y + 1) * L
    mx, my, mz = lax.axis_index("gx"), lax.axis_index("gy"), lax.axis_index("gz")
    lane = lax.broadcasted_iota(jnp.int32, (C, L), 1)

    def near(m, s, n):
        return lax.rem(m + (s + n), n)

    def side_id(sx, sy):
        out = {}
        if sx:
            out["gx"] = near(mx, sx, nx)
        if sy:
            out["gy"] = near(my, sy, ny)
        return out

    load_v = pltpu.make_async_copy(vol_ref, vin, in_sem.at[0])
    load_c = pltpu.make_async_copy(cot_ref, cin, in_sem.at[1])
    load_v.start()
    load_c.start()

    barrier = pltpu.get_barrier_semaphore()
    greets = 0
    for axis, m, n in (("gx", mx, nx), ("gy", my, ny), ("gz", mz, nz)):
        for d in range(1, n):
            pl.semaphore_signal(
                barrier, inc=1, device_id={axis: lax.rem(m + d, n)}, device_id_type=MESH
            )
            greets += 1
    for sx, sy in SIDES:
        if sx and sy:
            pl.semaphore_signal(barrier, inc=1, device_id=side_id(sx, sy), device_id_type=MESH)
            greets += 1

    def face(ref, sx, sy):
        src_x = {1: X, -1: 1, 0: pl.ds(1, X)}[sx]
        dst_x = {1: 0, -1: X + 1, 0: pl.ds(1, X)}[sx]
        src_y = {1: pl.ds(Y * L, L), -1: pl.ds(L, L), 0: pl.ds(I0, Y * L)}[sy]
        dst_y = {1: pl.ds(0, L), -1: pl.ds(I1, L), 0: pl.ds(I0, Y * L)}[sy]
        return ref.at[src_x, :, src_y], ref.at[dst_x, :, dst_y]

    def face_copy(which, ref, k):
        sx, sy = SIDES[k]
        src, dst = face(ref, sx, sy)
        return pltpu.make_async_remote_copy(
            src_ref=src, dst_ref=dst, send_sem=hsend.at[which, k], recv_sem=hrecv.at[which, k],
            device_id=side_id(sx, sy), device_id_type=MESH,
        )

    def col_copy(which, cb, h, k):
        s = 1 - 2 * k
        return pltpu.make_async_remote_copy(
            src_ref=cb.at[k], dst_ref=h.at[4, k],
            send_sem=hsend.at[which, 8 + k], recv_sem=hrecv.at[which, 8 + k],
            device_id={"gz": near(mz, s, nz)}, device_id_type=MESH,
        )

    def tile_copy(which, h, k):
        sx, sy = SIDES[k]
        return pltpu.make_async_remote_copy(
            src_ref=h.at[4], dst_ref=h.at[(1 - sx) * 3 + (1 - sy)],
            send_sem=hsend.at[which, 10 + k], recv_sem=hrecv.at[which, 10 + k],
            device_id=side_id(sx, sy), device_id_type=MESH,
        )

    def send_cols(which, cb, h):
        for k in range(2):
            col_copy(which, cb, h, k).start()

    def send_faces(which, e):
        for k in (1, 6, 3, 4, 0, 2, 5, 7):
            face_copy(which, e, k).start()

    def pass_tiles(which, cb, h):
        for k in range(2):
            col_copy(which, cb, h, k).wait_recv()
        for k in range(8):
            tile_copy(which, h, k).start()

    def wait_halo(which, e, h):
        for k in range(8):
            face_copy(which, e, k).wait_recv()
        for k in range(8):
            tile_copy(which, h, k).wait_recv()

    def drain_halo(which, e, cb, h):
        for k in range(8):
            face_copy(which, e, k).wait_send()
        for k in range(2):
            col_copy(which, cb, h, k).wait_send()
        for k in range(8):
            tile_copy(which, h, k).wait_send()

    def peer(buf, axis, m, n, ss, rs, d, arriving=False):
        slot = lax.rem(m + (n - d), n) if arriving else m
        return pltpu.make_async_remote_copy(
            src_ref=buf.at[m], dst_ref=buf.at[slot], send_sem=ss.at[d], recv_sem=rs.at[d],
            device_id={axis: lax.rem(m + d, n)}, device_id_type=MESH,
        )

    def arrive(buf, axis, m, n, ss, rs):
        for d in range(1, n):
            peer(buf, axis, m, n, ss, rs, d, True).wait_recv()

    def start(spec, value):
        buf, _, m, n = spec[:4]
        buf[m] = value
        for d in range(1, n):
            peer(*spec, d).start()

    def finish(spec):
        arrive(*spec)
        total = spec[0][0]
        for j in range(1, spec[3]):
            total = total + spec[0][j]
        return total

    def settle(spec):
        for d in range(1, spec[3]):
            peer(*spec, d).wait_send()

    stage = {
        (0, 0): (s1x, "gx", mx, nx, asend.at[0], arecv.at[0]),
        (0, 1): (s1y, "gy", my, ny, asend.at[1], arecv.at[1]),
        (0, 2): (s1z, "gz", mz, nz, asend.at[2], arecv.at[2]),
        (1, 0): (s2x, "gx", mx, nx, asend.at[3], arecv.at[3]),
        (1, 1): (s2y, "gy", my, ny, asend.at[4], arecv.at[4]),
        (1, 2): (s2z, "gz", mz, nz, asend.at[5], arecv.at[5]),
    }
    g_y = (gy_buf, "gy", my, ny, gsend.at[1], grecv.at[1])
    g_z = (gz_buf, "gz", mz, nz, gsend.at[2], grecv.at[2])
    g_f = (gf_buf, "gx", mx, nx, gsend.at[3], grecv.at[3])

    def pack(columns):
        tile = jnp.zeros((8, L), F32)
        lane8 = lane[0:8]
        for j, col in enumerate(columns):
            for half in range(2):
                tile = jnp.where(lane8 == 2 * j + half, col[8 * half : 8 * half + 8], tile)
        return tile

    def unpack(tile, j):
        lane8 = lane[0:8]
        return jnp.concatenate(
            [
                jnp.sum(jnp.where(lane8 == 2 * j + half, tile, 0.0), axis=1, keepdims=True)
                for half in range(2)
            ],
            axis=0,
        )

    def bring(src, e, cb):
        def body(x, cols):
            right, left = cols
            for y in range(Y):
                t = src[pl.ds(x * Y + y, C, stride=X * Y), :]
                e[x + 1, :, (y + 1) * L : (y + 2) * L] = t
                at = x * Y + y
                here = lane == at
                right = jnp.where(here, pltpu.roll(t, lax.rem(at + 1, L), 1), right)
                left = jnp.where(here, pltpu.roll(t, at, 1), left)
            return right, left

        zero = jnp.zeros((C, L), F32)
        right, left = lax.fori_loop(0, X, body, (zero, zero))
        cb[0] = right
        cb[1] = left

    def columns_of(e, cb):
        def body(x, cols):
            right, left = cols
            for y in range(Y):
                t = e[x + 1, :, (y + 1) * L : (y + 2) * L]
                at = x * Y + y
                here = lane == at
                right = jnp.where(here, pltpu.roll(t, lax.rem(at + 1, L), 1), right)
                left = jnp.where(here, pltpu.roll(t, at, 1), left)
            return right, left

        zero = jnp.zeros((C, L), F32)
        right, left = lax.fori_loop(0, X, body, (zero, zero))
        cb[0] = right
        cb[1] = left

    def build(e, h, xp, dx, xs, blocks):
        for yb in blocks:
            dy = -1 if yb == 0 else (1 if yb == Y + 1 else 0)
            ys = Y - 1 if yb == 0 else (0 if yb == Y + 1 else yb - 1)
            slot = (dx + 1) * 3 + dy + 1
            at = xs * Y + ys
            t = e[xp, :, yb * L : (yb + 1) * L]
            before = pltpu.roll(h[slot, 0], lax.rem(L - at, L), 1)
            after = pltpu.roll(h[slot, 1], lax.rem(2 * L - 1 - at, L), 1)
            low = jnp.where(lane == 0, before, pltpu.roll(t, 1, 1))
            high = jnp.where(lane == L - 1, after, pltpu.roll(t, L - 1, 1))
            for c, v in enumerate((low, t, high)):
                hi, lo = split(v)
                r_ref[xp, c * C : (c + 1) * C, yb * L : (yb + 1) * L] = hi
                r_ref[xp, (3 + c) * C : (4 + c) * C, yb * L : (yb + 1) * L] = lo

    def taps(xp, lo, hi):
        r = r_ref[xp, :, lo:hi]
        return jnp.concatenate([r, r[0 : 3 * C]], axis=0)

    def spread(m_ref, xp, lo, hi, which):
        part = jnp.dot(
            m_ref[which[0] * 3 * C : (which[-1] + 1) * 3 * C, :], taps(xp, lo, hi),
            preferred_element_type=F32,
        )
        for ia, a in enumerate(which):
            for b in range(3):
                row = (ia * 3 + b) * C
                at = lo + (2 - b) * L
                o_ref[xp - a + 2, :, at : at + hi - lo] += part[row : row + C]

    def clear():
        def body(x, carry):
            o_ref[x] = jnp.zeros((C, (Y + 4) * L), F32)
            return carry

        lax.fori_loop(0, X + 4, body, 0)

    def interior(m_ref, e, h):
        def body(x, carry):
            build(e, h, x + 1, 0, x, range(1, Y + 1))
            spread(m_ref, x + 1, I0, I1, (0, 1, 2))
            return carry

        lax.fori_loop(0, X, body, 0)

    def rim(m_ref, e, h):
        build(e, h, 0, -1, X - 1, range(Y + 2))
        spread(m_ref, 0, 0, W, (0,))
        build(e, h, X + 1, 1, 0, range(Y + 2))
        spread(m_ref, X + 1, 0, W, (2,))

        def body(x, carry):
            build(e, h, x + 1, 0, x, (0, Y + 1))
            spread(m_ref, x + 1, 0, L, (0, 1, 2))
            spread(m_ref, x + 1, I1, I1 + L, (0, 1, 2))
            return carry

        lax.fori_loop(0, X, body, 0)

    def clear_pad(ref):
        for x in range(X + 4):
            if x < 2 or x >= X + 2:
                ref[x] = jnp.zeros((2 * C, (Y + 4) * L), BF)
            else:
                ref[x, :, 0 : 2 * L] = jnp.zeros((2 * C, 2 * L), BF)
                ref[x, :, (Y + 2) * L : (Y + 4) * L] = jnp.zeros((2 * C, 2 * L), BF)

    def put_pad(ref, x, v):
        hi, lo = split(v)
        ref[x + 2, 0:C, 2 * L : (Y + 2) * L] = hi
        ref[x + 2, C : 2 * C, 2 * L : (Y + 2) * L] = lo

    def correlate(ref):
        acc_ref[...] = jnp.zeros((2 * ROWS, L), F32)

        def body(xp, carry):
            left = jnp.concatenate(
                [
                    ref[xp - a + 2, :, (2 - b) * L : (2 - b) * L + W]
                    for a in range(3)
                    for b in range(3)
                ],
                axis=0,
            )
            acc_ref[:, 0 : 6 * C] += lax.dot_general(
                left, r_ref[xp], (((1,), (1,)), ((), ())), preferred_element_type=F32
            )
            return carry

        lax.fori_loop(0, X + 2, body, 0)
        pieces = []
        for k in range(9):
            t = acc_ref[2 * k * C : (2 * k + 1) * C] + acc_ref[(2 * k + 1) * C : (2 * k + 2) * C]
            pieces.append(t + pltpu.roll(t, L - 3 * C, 1))
        return pieces

    clear()
    clear_pad(agp)
    clear_pad(cvp)
    load_v.wait()
    bring(vin, ev, cbv)
    pl.semaphore_wait(barrier, greets)
    send_cols(0, cbv, hv)
    send_faces(0, ev)
    load_c.wait()
    bring(cin, ec, cbc)
    pass_tiles(0, cbv, hv)
    send_cols(1, cbc, hc)
    send_faces(1, ec)
    interior(mf_ref, ev, hv)

    def vol_sum(x, s):
        return s + jnp.sum(ev[x + 1, :, I0:I1], axis=1, keepdims=True)

    in_sum = lax.fori_loop(0, X, vol_sum, jnp.zeros((C, 1), F32))
    wait_halo(0, ev, hv)
    rim(mf_ref, ev, hv)

    def gather_conv(x, sums):
        s, q = sums
        t = o_ref[x + 2, :, 2 * L : (Y + 2) * L]
        eo[x + 1, :, I0:I1] = t
        return (
            s + jnp.sum(t, axis=1, keepdims=True),
            q + jnp.sum(t * t, axis=1, keepdims=True),
        )

    zero_col = jnp.zeros((C, 1), F32)
    s, q = lax.fori_loop(0, X, gather_conv, (zero_col, zero_col))
    start(stage[0, 0], pack((s, q, in_sum)))
    columns_of(eo, cbo)
    send_cols(2, cbo, ho)
    send_faces(2, eo)

    def pad_conv(x, carry):
        put_pad(cvp, x, eo[x + 1, :, I0:I1])
        return carry

    lax.fori_loop(0, X, pad_conv, 0)
    part = finish(stage[0, 0])
    start(stage[0, 1], part)
    cross = correlate(cvp)
    for k in range(9):
        gw[k * C : (k + 1) * C] = pltpu.roll(cross[k], L // 2, 1)
    clear()
    pass_tiles(1, cbc, hc)
    part = finish(stage[0, 1])
    start(stage[0, 2], part)
    pass_tiles(2, cbo, ho)
    total1 = finish(stage[0, 2])
    mean = unpack(total1, 0) / count
    var = unpack(total1, 1) / count - mean * mean
    rstd = lax.rsqrt(var + 1e-05)
    gain = gain_ref[...]
    shift = shift_ref[...]

    def slope(conv, cot):
        normed = (conv - mean) * rstd
        act = gain * normed + shift
        sig = 1.0 / (1.0 + jnp.exp(-act))
        return cot * sig * (1.0 + act * (1.0 - sig)), normed

    def local_slope(x, sums):
        sg, sb = sums
        a, normed = slope(eo[x + 1, :, I0:I1], ec[x + 1, :, I0:I1])
        ea[x + 1, :, I0:I1] = a
        put_pad(agp, x, a)
        return (
            sg + jnp.sum(a * normed, axis=1, keepdims=True),
            sb + jnp.sum(a, axis=1, keepdims=True),
        )

    sg, sb = lax.fori_loop(0, X, local_slope, (zero_col, zero_col))
    start(stage[1, 0], pack((sg, sb)))
    cross = correlate(agp)
    for k in range(9):
        g = jnp.where(lane < L // 2, cross[k], gw[k * C : (k + 1) * C])
        gw[k * C : (k + 1) * C] = g
    tail = gw.shape[0] - ROWS
    if tail:
        gw[ROWS:] = jnp.zeros((tail, L), F32)
    chunk = gw.shape[0] // nx

    def piece(j):
        return gw.at[pl.ds(pl.multiple_of(j * chunk, 8), chunk)]

    gx_buf[mx] = gw[pl.ds(pl.multiple_of(mx * chunk, 8), chunk)]

    def scatter(d, arriving=False):
        to = lax.rem(mx + d, nx)
        slot = lax.rem(mx + (nx - d), nx) if arriving else mx
        return pltpu.make_async_remote_copy(
            src_ref=piece(to), dst_ref=gx_buf.at[slot],
            send_sem=gsend.at[0, d], recv_sem=grecv.at[0, d],
            device_id={"gx": to}, device_id_type=MESH,
        )

    part = finish(stage[1, 0])
    start(stage[1, 1], part)
    for d in range(1, nx):
        scatter(d).start()

    wait_halo(1, ec, hc)
    wait_halo(2, eo, ho)
    for xp in (0, X + 1):
        a, _ = slope(eo[xp], ec[xp])
        ea[xp] = a

    def edge_slope(x, carry):
        for at in (0, I1):
            a, _ = slope(eo[x + 1, :, at : at + L], ec[x + 1, :, at : at + L])
            ea[x + 1, :, at : at + L] = a
        return carry

    lax.fori_loop(0, X, edge_slope, 0)

    def tile_slope(k, carry):
        for j in range(2):
            a, _ = slope(ho[k, j], hc[k, j])
            ha[k, j] = a
        return carry

    lax.fori_loop(0, 9, tile_slope, 0)

    part = finish(stage[1, 1])
    start(stage[1, 2], part)
    for d in range(1, nx):
        scatter(d, True).wait_recv()
    gpart = gx_buf[0]
    for j in range(1, nx):
        gpart = gpart + gx_buf[j]
    start(g_y, gpart)
    total2 = finish(stage[1, 2])
    gain_grad = unpack(total2, 0)
    shift_grad = unpack(total2, 1)
    scale = gain * rstd
    k_conv = -scale * rstd * (gain_grad / count)
    k_one = -scale * (shift_grad / count) - k_conv * mean

    def blend(xp, carry):
        ea[xp] = scale * ea[xp] + k_conv * eo[xp] + k_one
        return carry

    lax.fori_loop(0, X + 2, blend, 0)

    def blend_tile(k, carry):
        for j in range(2):
            ha[k, j] = scale * ha[k, j] + k_conv * ho[k, j] + k_one
        return carry

    lax.fori_loop(0, 9, blend_tile, 0)
    gpart = finish(g_y)
    start(g_z, gpart)
    interior(mb_ref, ea, ha)
    gpart = finish(g_z)
    start(g_f, gpart)
    rim(mb_ref, ea, ha)

    def emit(x, carry):
        out_ref[x] = o_ref[x + 2, :, 2 * L : (Y + 2) * L]
        return carry

    lax.fori_loop(0, X, emit, 0)
    aux_ref[0:8] = total1
    aux_ref[8:16] = total2
    arrive(*g_f)
    for j in range(nx):
        aux_ref[16 + j * chunk : 16 + (j + 1) * chunk] = gf_buf[j]

    drain_halo(0, ev, cbv, hv)
    drain_halo(1, ec, cbc, hc)
    drain_halo(2, eo, cbo, ho)
    for key in stage:
        settle(stage[key])
    for d in range(1, nx):
        scatter(d).wait_send()
    for spec in (g_y, g_z, g_f):
        settle(spec)


def shards(sizes, volume, weight, gamma, beta, cotangent):
    nx, ny, nz = sizes
    _, X, Y, Z = volume.shape
    count = float(X * Y * Z * nx * ny * nz)
    W = (Y + 2) * L
    chunk = -(-(ROWS // 8) // nx) * 8
    rows = chunk * nx

    def stack(w):
        hi = w.astype(BF).astype(F32)
        lo = w - hi
        return jnp.concatenate([hi, hi, lo], axis=1).astype(BF)

    forward = stack(weight.transpose(2, 3, 0, 4, 1).reshape(ROWS, 3 * C))
    backward = stack(
        weight[:, :, ::-1, ::-1, ::-1].transpose(2, 3, 1, 4, 0).reshape(ROWS, 3 * C)
    )
    vmem = pl.BlockSpec(memory_space=pltpu.VMEM)
    hbm = pl.BlockSpec(memory_space=pl.ANY)
    e_shape = pltpu.VMEM((X + 2, C, W), F32)
    h_shape = pltpu.VMEM((9, 2, C, L), F32)
    cb_shape = pltpu.VMEM((2, C, L), F32)
    pad_shape = pltpu.VMEM((X + 4, 2 * C, (Y + 4) * L), BF)
    dma = pltpu.SemaphoreType.DMA
    most = max(nx, ny, nz)
    blocks, aux = pl.pallas_call(
        functools.partial(kernel, (nx, ny, nz, X, Y), count),
        out_shape=(
            jax.ShapeDtypeStruct((X, C, Y * L), F32),
            jax.ShapeDtypeStruct((16 + rows, L), F32),
        ),
        in_specs=[hbm, hbm, vmem, vmem, vmem, vmem],
        out_specs=(vmem, vmem),
        scratch_shapes=[
            pltpu.VMEM((C * X * Y, L), F32), pltpu.VMEM((C * X * Y, L), F32),
            e_shape, e_shape, e_shape, e_shape,
            h_shape, h_shape, h_shape, h_shape,
            cb_shape, cb_shape, cb_shape,
            pltpu.VMEM((X + 2, 6 * C, W), BF),
            pltpu.VMEM((X + 4, C, (Y + 4) * L), F32),
            pad_shape, pad_shape,
            pltpu.VMEM((2 * ROWS, L), F32),
            pltpu.VMEM((rows, L), F32),
            pltpu.VMEM((nx, 8, L), F32), pltpu.VMEM((ny, 8, L), F32), pltpu.VMEM((nz, 8, L), F32),
            pltpu.VMEM((nx, 8, L), F32), pltpu.VMEM((ny, 8, L), F32), pltpu.VMEM((nz, 8, L), F32),
            pltpu.VMEM((nx, chunk, L), F32), pltpu.VMEM((ny, chunk, L), F32),
            pltpu.VMEM((nz, chunk, L), F32), pltpu.VMEM((nx, chunk, L), F32),
            dma((2,)), dma((3, 18)), dma((3, 18)), dma((6, most)), dma((6, most)),
            dma((4, most)), dma((4, most)),
        ],
        compiler_params=pltpu.CompilerParams(
            collective_id=0, has_side_effects=True, vmem_limit_bytes=60 << 20
        ),
    )(
        volume.reshape(C * X * Y, L), cotangent.reshape(C * X * Y, L), forward, backward,
        gamma.reshape(C, 1), beta.reshape(C, 1),
    )
    input_grad = blocks.reshape(X, C, Y, L).transpose(1, 0, 2, 3)

    def column(base, j):
        return jnp.concatenate([aux[base : base + 8, 2 * j], aux[base : base + 8, 2 * j + 1]])

    mean = column(0, 0) / count
    var = column(0, 1) / count - mean * mean
    input_total = column(0, 2)
    rstd = lax.rsqrt(var + 1e-05)
    gamma_grad = column(8, 0)
    beta_grad = column(8, 1)
    scale = gamma * rstd
    both = aux[16 : 16 + ROWS]

    def taps(lo):
        return both[:, lo : lo + 3 * C].reshape(3, 3, C, 3, C).transpose(2, 4, 0, 1, 3)

    def out(v):
        return v[:, None, None, None, None]

    wide = input_total[None, :, None, None, None]
    norm_total = out(rstd) * (taps(L // 2) - out(mean) * wide)
    weight_grad = out(scale) * (
        taps(0) - out(beta_grad / count) * wide - out(gamma_grad / count) * norm_total
    )
    return (input_grad, weight_grad, gamma_grad, beta_grad)


def solution(mesh):
    sizes = tuple(mesh.shape[name] for name in ("gx", "gy", "gz"))
    spec = P(None, "gx", "gy", "gz")
    return jax.shard_map(
        functools.partial(shards, sizes),
        mesh=mesh,
        in_specs=(spec, P(), P(), P(), spec),
        out_specs=(spec, P(), P(), P()),
        check_vma=False,
    )
```

```python
import functools

import jax
import jax.numpy as jnp
from jax import lax
from jax.experimental import pallas as pl
from jax.experimental.pallas import tpu as pltpu
from jax.sharding import PartitionSpec as P

MESH = pl.DeviceIdType.MESH
L = 128
C = 16
ROWS = 9 * C
BF = jnp.bfloat16
F32 = jnp.float32
SIDES = [(sx, sy) for sx in (-1, 0, 1) for sy in (-1, 0, 1) if (sx, sy) != (0, 0)]


def split(v):
    hi = v.astype(BF)
    lo = (v - hi.astype(F32)).astype(BF)
    return hi, lo


def kernel(
    dims, count, vol_ref, cot_ref, w_ref, gain_ref, shift_ref,
    out_ref, wout_ref, gout_ref, bout_ref,
    vin, cin, wv, gv, bv, mf_ref, mb_ref, ev, ec, eo, ea, hv, hc, ho, ha, cbv, cbc, cbo,
    r_ref, o_ref, agp, cvp, acc_ref, gw, gfull,
    z1, p1, z2, p2, gp_buf, gy_buf, gf_buf,
    in_sem, hsend, hrecv, asend, arecv, gsend, grecv,
):
    nx, ny, nz, X, Y = dims
    W = (Y + 2) * L
    I0, I1 = L, (Y + 1) * L
    mx, my, mz = lax.axis_index("gx"), lax.axis_index("gy"), lax.axis_index("gz")
    lane = lax.broadcasted_iota(jnp.int32, (C, L), 1)
    sub = lax.broadcasted_iota(jnp.int32, (C, L), 0)
    half = L // 2
    npl = nx * nz
    mp = mx * nz + mz

    def plane_id(q):
        return {"gx": lax.div(q, nz), "gz": lax.rem(q, nz)}

    def line_id(q):
        return {"gy": q}

    plane = (plane_id, mp, npl)
    line = (line_id, my, ny)

    def near(m, s, n):
        return lax.rem(m + (s + n), n)

    def side_id(sx, sy):
        out = {}
        if sx:
            out["gx"] = near(mx, sx, nx)
        if sy:
            out["gy"] = near(my, sy, ny)
        return out

    loads = [
        pltpu.make_async_copy(src, dst, in_sem.at[k])
        for k, (src, dst) in enumerate(
            ((vol_ref, vin), (cot_ref, cin), (w_ref, wv), (gain_ref, gv), (shift_ref, bv))
        )
    ]
    for copy in loads:
        copy.start()

    barrier = pltpu.get_barrier_semaphore()
    greets = 0
    for name, m, n in (plane, line):
        for d in range(1, n):
            pl.semaphore_signal(
                barrier, inc=1, device_id=name(lax.rem(m + d, n)), device_id_type=MESH
            )
            greets += 1
    for sx, sy in SIDES:
        if sx and sy:
            pl.semaphore_signal(barrier, inc=1, device_id=side_id(sx, sy), device_id_type=MESH)
            greets += 1

    def face(ref, sx, sy):
        src_x = {1: X, -1: 1, 0: pl.ds(1, X)}[sx]
        dst_x = {1: 0, -1: X + 1, 0: pl.ds(1, X)}[sx]
        src_y = {1: pl.ds(Y * L, L), -1: pl.ds(L, L), 0: pl.ds(I0, Y * L)}[sy]
        dst_y = {1: pl.ds(0, L), -1: pl.ds(I1, L), 0: pl.ds(I0, Y * L)}[sy]
        return ref.at[src_x, :, src_y], ref.at[dst_x, :, dst_y]

    def face_copy(which, ref, k):
        sx, sy = SIDES[k]
        src, dst = face(ref, sx, sy)
        return pltpu.make_async_remote_copy(
            src_ref=src, dst_ref=dst, send_sem=hsend.at[which, k], recv_sem=hrecv.at[which, k],
            device_id=side_id(sx, sy), device_id_type=MESH,
        )

    def col_copy(which, cb, k):
        s = 1 - 2 * k
        return pltpu.make_async_remote_copy(
            src_ref=cb.at[k], dst_ref=cb.at[2 + k],
            send_sem=hsend.at[which, 8 + k], recv_sem=hrecv.at[which, 8 + k],
            device_id={"gz": near(mz, s, nz)}, device_id_type=MESH,
        )

    def tile_copy(which, h, k):
        sx, sy = SIDES[k]
        return pltpu.make_async_remote_copy(
            src_ref=h.at[4], dst_ref=h.at[(1 - sx) * 3 + (1 - sy)],
            send_sem=hsend.at[which, 10 + k], recv_sem=hrecv.at[which, 10 + k],
            device_id=side_id(sx, sy), device_id_type=MESH,
        )

    def send_cols(which, cb):
        for k in range(2):
            col_copy(which, cb, k).start()

    def send_faces(which, e):
        for k in (1, 6, 3, 4, 0, 2, 5, 7):
            face_copy(which, e, k).start()

    def pass_tiles(which, cb, h):
        for k in range(2):
            col_copy(which, cb, k).wait_recv()
        h[4] = jnp.where(lane < half, cb[2], cb[3])
        for k in range(8):
            tile_copy(which, h, k).start()

    def wait_halo(which, e, h):
        for k in range(8):
            face_copy(which, e, k).wait_recv()
        for k in range(8):
            tile_copy(which, h, k).wait_recv()

    def drain_halo(which, e, cb, h):
        for k in range(8):
            face_copy(which, e, k).wait_send()
        for k in range(2):
            col_copy(which, cb, k).wait_send()
        for k in range(8):
            tile_copy(which, h, k).wait_send()

    def peer(buf, group, ss, rs, d, arriving=False):
        name, m, n = group
        slot = lax.rem(m + (n - d), n) if arriving else m
        return pltpu.make_async_remote_copy(
            src_ref=buf.at[m], dst_ref=buf.at[slot], send_sem=ss.at[d], recv_sem=rs.at[d],
            device_id=name(lax.rem(m + d, n)), device_id_type=MESH,
        )

    def arrive(buf, group, ss, rs):
        for d in range(1, group[2]):
            peer(buf, group, ss, rs, d, True).wait_recv()

    def start(spec, value):
        spec[0][spec[1][1]] = value
        for d in range(1, spec[1][2]):
            peer(*spec, d).start()

    def finish(spec):
        arrive(*spec)
        total = spec[0][0]
        for j in range(1, spec[1][2]):
            total = total + spec[0][j]
        return total

    def settle(spec):
        for d in range(1, spec[1][2]):
            peer(*spec, d).wait_send()

    s_z1 = (z1, line, asend.at[0], arecv.at[0])
    s_p1 = (p1, plane, asend.at[1], arecv.at[1])
    s_z2 = (z2, line, asend.at[2], arecv.at[2])
    s_p2 = (p2, plane, asend.at[3], arecv.at[3])
    g_y = (gy_buf, line, gsend.at[1], grecv.at[1])
    g_f = (gf_buf, plane, gsend.at[2], grecv.at[2])

    def pack(columns):
        tile = jnp.zeros((C, L), F32)
        for j, col in enumerate(columns):
            tile = jnp.where(lane == sub + j * C, col, tile)
        return jnp.sum(tile, axis=0, keepdims=True)

    def unpack(row, j):
        return jnp.sum(jnp.where(lane == sub + j * C, row, 0.0), axis=1, keepdims=True)

    def bring(src, e, cb):
        def body(x, cols):
            right, left = cols
            for y in range(Y):
                t = src[pl.ds(x * Y + y, C, stride=X * Y), :]
                e[x + 1, :, (y + 1) * L : (y + 2) * L] = t
                at = x * Y + y
                right = jnp.where(lane == at, pltpu.roll(t, at + 1, 1), right)
                left = jnp.where(lane == at + half, pltpu.roll(t, at + half, 1), left)
            return right, left

        zero = jnp.zeros((C, L), F32)
        right, left = lax.fori_loop(0, X, body, (zero, zero))
        cb[0] = right
        cb[1] = left

    def columns_of(e, cb):
        def body(x, cols):
            right, left = cols
            for y in range(Y):
                t = e[x + 1, :, (y + 1) * L : (y + 2) * L]
                at = x * Y + y
                right = jnp.where(lane == at, pltpu.roll(t, at + 1, 1), right)
                left = jnp.where(lane == at + half, pltpu.roll(t, at + half, 1), left)
            return right, left

        zero = jnp.zeros((C, L), F32)
        right, left = lax.fori_loop(0, X, body, (zero, zero))
        cb[0] = right
        cb[1] = left

    def build(e, h, xp, dx, xs, blocks):
        for yb in blocks:
            dy = -1 if yb == 0 else (1 if yb == Y + 1 else 0)
            ys = Y - 1 if yb == 0 else (0 if yb == Y + 1 else yb - 1)
            slot = (dx + 1) * 3 + dy + 1
            at = xs * Y + ys
            t = e[xp, :, yb * L : (yb + 1) * L]
            before = pltpu.roll(h[slot], lax.rem(L - at, L), 1)
            after = pltpu.roll(h[slot], half - 1 - at, 1)
            low = jnp.where(lane == 0, before, pltpu.roll(t, 1, 1))
            high = jnp.where(lane == L - 1, after, pltpu.roll(t, L - 1, 1))
            for c, v in enumerate((low, t, high)):
                hi, lo = split(v)
                r_ref[xp, c * C : (c + 1) * C, yb * L : (yb + 1) * L] = hi
                r_ref[xp, (3 + c) * C : (4 + c) * C, yb * L : (yb + 1) * L] = lo

    def taps(xp, lo, hi):
        r = r_ref[xp, :, lo:hi]
        return jnp.concatenate([r, r[0 : 3 * C]], axis=0)

    def spread(m_ref, xp, lo, hi, which):
        part = jnp.dot(
            m_ref[which[0] * 3 * C : (which[-1] + 1) * 3 * C, :], taps(xp, lo, hi),
            preferred_element_type=F32,
        )
        for ia, a in enumerate(which):
            for b in range(3):
                row = (ia * 3 + b) * C
                at = lo + (2 - b) * L
                o_ref[xp - a + 2, :, at : at + hi - lo] += part[row : row + C]

    def clear():
        def body(x, carry):
            o_ref[x] = jnp.zeros((C, (Y + 4) * L), F32)
            return carry

        lax.fori_loop(0, X + 4, body, 0)

    def interior(m_ref, e, h):
        def body(x, carry):
            build(e, h, x + 1, 0, x, range(1, Y + 1))
            spread(m_ref, x + 1, I0, I1, (0, 1, 2))
            return carry

        lax.fori_loop(0, X, body, 0)

    def rim(m_ref, e, h):
        build(e, h, 0, -1, X - 1, range(Y + 2))
        spread(m_ref, 0, 0, W, (0,))
        build(e, h, X + 1, 1, 0, range(Y + 2))
        spread(m_ref, X + 1, 0, W, (2,))

        def body(x, carry):
            build(e, h, x + 1, 0, x, (0, Y + 1))
            spread(m_ref, x + 1, 0, L, (0, 1, 2))
            spread(m_ref, x + 1, I1, I1 + L, (0, 1, 2))
            return carry

        lax.fori_loop(0, X, body, 0)

    def clear_pad(ref):
        for x in range(X + 4):
            if x < 2 or x >= X + 2:
                ref[x] = jnp.zeros((2 * C, (Y + 4) * L), BF)
            else:
                ref[x, :, 0 : 2 * L] = jnp.zeros((2 * C, 2 * L), BF)
                ref[x, :, (Y + 2) * L : (Y + 4) * L] = jnp.zeros((2 * C, 2 * L), BF)

    def put_pad(ref, x, v):
        hi, lo = split(v)
        ref[x + 2, 0:C, 2 * L : (Y + 2) * L] = hi
        ref[x + 2, C : 2 * C, 2 * L : (Y + 2) * L] = lo

    def correlate(ref):
        acc_ref[...] = jnp.zeros((2 * ROWS, L), F32)

        def body(xp, carry):
            left = jnp.concatenate(
                [
                    ref[xp - a + 2, :, (2 - b) * L : (2 - b) * L + W]
                    for a in range(3)
                    for b in range(3)
                ],
                axis=0,
            )
            acc_ref[:, 0 : 6 * C] += lax.dot_general(
                left, r_ref[xp], (((1,), (1,)), ((), ())), preferred_element_type=F32
            )
            return carry

        lax.fori_loop(0, X + 2, body, 0)
        pieces = []
        for k in range(9):
            t = acc_ref[2 * k * C : (2 * k + 1) * C] + acc_ref[(2 * k + 1) * C : (2 * k + 2) * C]
            pieces.append(t + pltpu.roll(t, L - 3 * C, 1))
        return pieces

    def put_weights(m_ref, k, t):
        hi = t.astype(BF).astype(F32)
        m_ref[k * C : (k + 1) * C, :] = jnp.concatenate([hi, hi, t - hi], axis=1).astype(BF)

    def weights_forward():
        for k in range(9):
            at = k * 3 * C
            put_weights(
                mf_ref, k,
                jnp.concatenate([wv[at + c * C : at + (c + 1) * C] for c in range(3)], axis=1),
            )

    def weights_backward():
        for k in range(9):
            at = (8 - k) * 3 * C
            put_weights(
                mb_ref, k,
                jnp.concatenate(
                    [wv[at + c * C : at + (c + 1) * C] for c in (2, 1, 0)], axis=0
                ).T,
            )

    def as_column(ref):
        square = lax.broadcasted_iota(jnp.int32, (C, C), 0) == lax.broadcasted_iota(
            jnp.int32, (C, C), 1
        )
        return jnp.sum(jnp.where(square, ref[...], 0.0), axis=1, keepdims=True)

    loads[0].wait()
    bring(vin, ev, cbv)
    pl.semaphore_wait(barrier, greets)
    send_cols(0, cbv)
    send_faces(0, ev)
    for copy in loads[1:]:
        copy.wait()
    clear()
    weights_forward()
    bring(cin, ec, cbc)
    pass_tiles(0, cbv, hv)
    send_cols(1, cbc)
    send_faces(1, ec)
    interior(mf_ref, ev, hv)
    clear_pad(agp)
    clear_pad(cvp)
    weights_backward()

    def vol_sum(x, s):
        return s + jnp.sum(ev[x + 1, :, I0:I1], axis=1, keepdims=True)

    in_sum = lax.fori_loop(0, X, vol_sum, jnp.zeros((C, 1), F32))
    wait_halo(0, ev, hv)
    rim(mf_ref, ev, hv)

    def gather_conv(x, sums):
        s, q = sums
        t = o_ref[x + 2, :, 2 * L : (Y + 2) * L]
        eo[x + 1, :, I0:I1] = t
        return (
            s + jnp.sum(t, axis=1, keepdims=True),
            q + jnp.sum(t * t, axis=1, keepdims=True),
        )

    zero_col = jnp.zeros((C, 1), F32)
    s, q = lax.fori_loop(0, X, gather_conv, (zero_col, zero_col))
    start(s_z1, pack((s, q, in_sum)))
    columns_of(eo, cbo)
    send_cols(2, cbo)

    def pad_conv(x, carry):
        put_pad(cvp, x, eo[x + 1, :, I0:I1])
        return carry

    lax.fori_loop(0, X, pad_conv, 0)
    part = finish(s_z1)
    start(s_p1, part)
    send_faces(2, eo)
    pass_tiles(1, cbc, hc)
    cross = correlate(cvp)
    for k in range(9):
        gw[k * C : (k + 1) * C] = pltpu.roll(cross[k], half, 1)
    pass_tiles(2, cbo, ho)
    clear()
    gain = as_column(gv)
    shift = as_column(bv)
    total1 = finish(s_p1)
    mean = unpack(total1, 0) / count
    var = unpack(total1, 1) / count - mean * mean
    rstd = lax.rsqrt(var + 1e-05)

    def slope(conv, cot):
        normed = (conv - mean) * rstd
        act = gain * normed + shift
        sig = 1.0 / (1.0 + jnp.exp(-act))
        return cot * sig * (1.0 + act * (1.0 - sig)), normed

    def local_slope(x, sums):
        sg, sb = sums
        a, normed = slope(eo[x + 1, :, I0:I1], ec[x + 1, :, I0:I1])
        ea[x + 1, :, I0:I1] = a
        put_pad(agp, x, a)
        return (
            sg + jnp.sum(a * normed, axis=1, keepdims=True),
            sb + jnp.sum(a, axis=1, keepdims=True),
        )

    sg, sb = lax.fori_loop(0, X, local_slope, (zero_col, zero_col))
    start(s_z2, pack((sg, sb)))
    cross = correlate(agp)
    for k in range(9):
        gw[k * C : (k + 1) * C] = jnp.where(lane < half, cross[k], gw[k * C : (k + 1) * C])
    if gw.shape[0] > ROWS:
        gw[ROWS:] = jnp.zeros((gw.shape[0] - ROWS, L), F32)
    chunk = gw.shape[0] // npl

    def piece(j):
        return gw.at[pl.ds(pl.multiple_of(j * chunk, 8), chunk)]

    def scatter(d, arriving=False):
        to = lax.rem(mp + d, npl)
        slot = lax.rem(mp + (npl - d), npl) if arriving else mp
        return pltpu.make_async_remote_copy(
            src_ref=piece(to), dst_ref=gp_buf.at[slot],
            send_sem=gsend.at[0, d], recv_sem=grecv.at[0, d],
            device_id=plane_id(to), device_id_type=MESH,
        )

    part = finish(s_z2)
    start(s_p2, part)
    gp_buf[mp] = gw[pl.ds(pl.multiple_of(mp * chunk, 8), chunk)]
    for d in range(1, npl):
        scatter(d).start()

    wait_halo(1, ec, hc)
    wait_halo(2, eo, ho)
    for xp in (0, X + 1):
        a, _ = slope(eo[xp], ec[xp])
        ea[xp] = a

    def edge_slope(x, carry):
        for at in (0, I1):
            a, _ = slope(eo[x + 1, :, at : at + L], ec[x + 1, :, at : at + L])
            ea[x + 1, :, at : at + L] = a
        return carry

    lax.fori_loop(0, X, edge_slope, 0)

    def tile_slope(k, carry):
        a, _ = slope(ho[k], hc[k])
        ha[k] = a
        return carry

    lax.fori_loop(0, 9, tile_slope, 0)

    total2 = finish(s_p2)
    for d in range(1, npl):
        scatter(d, True).wait_recv()
    gpart = gp_buf[0]
    for j in range(1, npl):
        gpart = gpart + gp_buf[j]
    start(g_y, gpart)
    gain_grad = unpack(total2, 0)
    shift_grad = unpack(total2, 1)
    scale = gain * rstd
    k_conv = -scale * rstd * (gain_grad / count)
    k_one = -scale * (shift_grad / count) - k_conv * mean

    def blend(xp, carry):
        ea[xp] = scale * ea[xp] + k_conv * eo[xp] + k_one
        return carry

    lax.fori_loop(0, X + 2, blend, 0)

    def blend_tile(k, carry):
        ha[k] = scale * ha[k] + k_conv * ho[k] + k_one
        return carry

    lax.fori_loop(0, 9, blend_tile, 0)
    interior(mb_ref, ea, ha)
    gpart = finish(g_y)
    start(g_f, gpart)
    rim(mb_ref, ea, ha)

    def emit(x, carry):
        for y in range(Y):
            out_ref[pl.ds(x * Y + y, C, stride=X * Y), :] = o_ref[
                x + 2, :, (y + 2) * L : (y + 3) * L
            ]
        return carry

    lax.fori_loop(0, X, emit, 0)
    gout_ref[...] = total2[:, 0:C]
    bout_ref[...] = pltpu.roll(total2, L - C, 1)[:, 0:C]
    wide = jnp.sum(
        jnp.where(lax.rem(lane, C) == sub, unpack(total1, 2), 0.0), axis=0, keepdims=True
    )
    arrive(*g_f)
    for j in range(npl):
        gfull[j * chunk : (j + 1) * chunk] = gf_buf[j]
    for k in range(9):
        t = gfull[k * C : (k + 1) * C]
        norm = rstd * (pltpu.roll(t, half, 1) - mean * wide)
        t = scale * (t - (shift_grad / count) * wide - (gain_grad / count) * norm)
        for c in range(3):
            at = (k * 3 + c) * C
            wout_ref[at : at + C, :] = (t if c == 0 else pltpu.roll(t, L - c * C, 1))[:, 0:C]

    drain_halo(0, ev, cbv, hv)
    drain_halo(1, ec, cbc, hc)
    drain_halo(2, eo, cbo, ho)
    for spec in (s_z1, s_p1, s_z2, s_p2, g_y, g_f):
        settle(spec)
    for d in range(1, npl):
        scatter(d).wait_send()


def shards(sizes, volume, weight, gamma, beta, cotangent):
    nx, ny, nz = sizes
    _, X, Y, Z = volume.shape
    count = float(X * Y * Z * nx * ny * nz)
    W = (Y + 2) * L
    npl = nx * nz
    chunk = -(-(ROWS // 8) // npl) * 8
    rows = chunk * npl
    vmem = pl.BlockSpec(memory_space=pltpu.VMEM)
    hbm = pl.BlockSpec(memory_space=pl.ANY)
    e_shape = pltpu.VMEM((X + 2, C, W), F32)
    h_shape = pltpu.VMEM((9, C, L), F32)
    cb_shape = pltpu.VMEM((4, C, L), F32)
    pad_shape = pltpu.VMEM((X + 4, 2 * C, (Y + 4) * L), BF)
    m_shape = pltpu.VMEM((ROWS, ROWS), BF)
    line_rows = pltpu.VMEM((ny, 1, L), F32)
    plane_rows = pltpu.VMEM((npl, 1, L), F32)
    dma = pltpu.SemaphoreType.DMA
    most = max(npl, ny)
    flat, wflat, gain_grad, shift_grad = pl.pallas_call(
        functools.partial(kernel, (nx, ny, nz, X, Y), count),
        out_shape=(
            jax.ShapeDtypeStruct((C * X * Y, L), F32),
            jax.ShapeDtypeStruct((27 * C, C), F32),
            jax.ShapeDtypeStruct((1, C), F32),
            jax.ShapeDtypeStruct((1, C), F32),
        ),
        in_specs=[hbm, hbm, hbm, hbm, hbm],
        out_specs=(vmem, vmem, vmem, vmem),
        scratch_shapes=[
            pltpu.VMEM((C * X * Y, L), F32), pltpu.VMEM((C * X * Y, L), F32),
            pltpu.VMEM((27 * C, C), F32), pltpu.VMEM((1, C), F32), pltpu.VMEM((1, C), F32),
            m_shape, m_shape,
            e_shape, e_shape, e_shape, e_shape,
            h_shape, h_shape, h_shape, h_shape,
            cb_shape, cb_shape, cb_shape,
            pltpu.VMEM((X + 2, 6 * C, W), BF),
            pltpu.VMEM((X + 4, C, (Y + 4) * L), F32),
            pad_shape, pad_shape,
            pltpu.VMEM((2 * ROWS, L), F32),
            pltpu.VMEM((rows, L), F32), pltpu.VMEM((rows, L), F32),
            line_rows, plane_rows, line_rows, plane_rows,
            pltpu.VMEM((npl, chunk, L), F32), pltpu.VMEM((ny, chunk, L), F32),
            pltpu.VMEM((npl, chunk, L), F32),
            dma((5,)), dma((3, 18)), dma((3, 18)), dma((4, most)), dma((4, most)),
            dma((3, most)), dma((3, most)),
        ],
        compiler_params=pltpu.CompilerParams(
            collective_id=0, has_side_effects=True, vmem_limit_bytes=60 << 20
        ),
    )(
        volume.reshape(C * X * Y, L), cotangent.reshape(C * X * Y, L),
        weight.transpose(2, 3, 4, 0, 1).reshape(27 * C, C),
        gamma.reshape(1, C), beta.reshape(1, C),
    )
    return (
        flat.reshape(C, X, Y, Z),
        wflat.reshape(3, 3, 3, C, C).transpose(3, 4, 0, 1, 2),
        gain_grad.reshape(C),
        shift_grad.reshape(C),
    )


def solution(mesh):
    sizes = tuple(mesh.shape[name] for name in ("gx", "gy", "gz"))
    spec = P(None, "gx", "gy", "gz")
    return jax.shard_map(
        functools.partial(shards, sizes),
        mesh=mesh,
        in_specs=(spec, P(), P(), P(), spec),
        out_specs=(spec, P(), P(), P()),
        check_vma=False,
    )
```

```python
import functools

import jax
import jax.numpy as jnp
from jax import lax
from jax.experimental import pallas as pl
from jax.experimental.pallas import tpu as pltpu
from jax.sharding import PartitionSpec as P

MESH = pl.DeviceIdType.MESH
L = 128
C = 16
ROWS = 9 * C
BF = jnp.bfloat16
F32 = jnp.float32
SIDES = [(sx, sy) for sx in (-1, 0, 1) for sy in (-1, 0, 1) if (sx, sy) != (0, 0)]


def split(v):
    hi = v.astype(BF)
    lo = (v - hi.astype(F32)).astype(BF)
    return hi, lo


def kernel(
    dims, count, vol_ref, cot_ref, w_ref, gain_ref, shift_ref,
    out_ref, wout_ref, gout_ref, bout_ref,
    vin, cin, wv, gv, bv, mf_ref, mb_ref, ev, ec, eo, ea, hv, hc, ho, ha, cbv, cbc, cbo,
    r_ref, o_ref, agp, cvp, acc_ref, gw, gfull,
    z1, p1, z2, p2, gp_buf, gy_buf, gf_buf,
    in_sem, hsend, hrecv, asend, arecv, gsend, grecv,
):
    nx, ny, nz, X, Y = dims
    W = (Y + 2) * L
    I0, I1 = L, (Y + 1) * L
    mx, my, mz = lax.axis_index("gx"), lax.axis_index("gy"), lax.axis_index("gz")
    lane = lax.broadcasted_iota(jnp.int32, (C, L), 1)
    sub = lax.broadcasted_iota(jnp.int32, (C, L), 0)
    half = L // 2
    npl = nx * nz
    xs_at = [mx] + [lax.rem(mx + d, nx) for d in range(1, nx)]
    ys_at = [my] + [lax.rem(my + d, ny) for d in range(1, ny)]
    zs_at = [mz] + [lax.rem(mz + d, nz) for d in range(1, nz)]
    xs_row = [x * nz for x in xs_at]
    mp = xs_row[0] + mz
    plane = (
        mp, npl,
        [
            (
                dx * nz + dz, {"gx": xs_at[dx], "gz": zs_at[dz]},
                xs_row[dx] + zs_at[dz], xs_row[-dx] + zs_at[-dz],
            )
            for dx in range(nx)
            for dz in range(nz)
            if dx or dz
        ],
    )
    line = (my, ny, [(d, {"gy": ys_at[d]}, ys_at[d], ys_at[-d]) for d in range(1, ny)])

    def side_id(sx, sy):
        out = {}
        if sx:
            out["gx"] = xs_at[sx]
        if sy:
            out["gy"] = ys_at[sy]
        return out

    loads = [
        pltpu.make_async_copy(src, dst, in_sem.at[k])
        for k, (src, dst) in enumerate(
            ((vol_ref, vin), (cot_ref, cin), (w_ref, wv), (gain_ref, gv), (shift_ref, bv))
        )
    ]
    for copy in loads:
        copy.start()

    barrier = pltpu.get_barrier_semaphore()
    greets = 0
    for group in (plane, line):
        for _, there, _, _ in group[2]:
            pl.semaphore_signal(barrier, inc=1, device_id=there, device_id_type=MESH)
            greets += 1
    for sx, sy in SIDES:
        if sx and sy:
            pl.semaphore_signal(barrier, inc=1, device_id=side_id(sx, sy), device_id_type=MESH)
            greets += 1

    def face(ref, sx, sy):
        src_x = {1: X, -1: 1, 0: pl.ds(1, X)}[sx]
        dst_x = {1: 0, -1: X + 1, 0: pl.ds(1, X)}[sx]
        src_y = {1: pl.ds(Y * L, L), -1: pl.ds(L, L), 0: pl.ds(I0, Y * L)}[sy]
        dst_y = {1: pl.ds(0, L), -1: pl.ds(I1, L), 0: pl.ds(I0, Y * L)}[sy]
        return ref.at[src_x, :, src_y], ref.at[dst_x, :, dst_y]

    def face_copy(which, ref, k):
        sx, sy = SIDES[k]
        src, dst = face(ref, sx, sy)
        return pltpu.make_async_remote_copy(
            src_ref=src, dst_ref=dst, send_sem=hsend.at[which, k], recv_sem=hrecv.at[which, k],
            device_id=side_id(sx, sy), device_id_type=MESH,
        )

    def col_copy(which, cb, k):
        s = 1 - 2 * k
        return pltpu.make_async_remote_copy(
            src_ref=cb.at[k], dst_ref=cb.at[2 + k],
            send_sem=hsend.at[which, 8 + k], recv_sem=hrecv.at[which, 8 + k],
            device_id={"gz": zs_at[s]}, device_id_type=MESH,
        )

    def tile_copy(which, h, k):
        sx, sy = SIDES[k]
        return pltpu.make_async_remote_copy(
            src_ref=h.at[4], dst_ref=h.at[(1 - sx) * 3 + (1 - sy)],
            send_sem=hsend.at[which, 10 + k], recv_sem=hrecv.at[which, 10 + k],
            device_id=side_id(sx, sy), device_id_type=MESH,
        )

    def send_cols(which, cb):
        for k in range(2):
            col_copy(which, cb, k).start()

    def send_faces(which, e):
        for k in (1, 6, 3, 4, 0, 2, 5, 7):
            face_copy(which, e, k).start()

    def pass_tiles(which, cb, h):
        for k in range(2):
            col_copy(which, cb, k).wait_recv()
        h[4] = jnp.where(lane < half, cb[2], cb[3])
        for k in range(8):
            tile_copy(which, h, k).start()

    def wait_halo(which, e, h):
        for k in range(8):
            face_copy(which, e, k).wait_recv()
        for k in range(8):
            tile_copy(which, h, k).wait_recv()

    def drain_halo(which, e, cb, h):
        for k in range(8):
            face_copy(which, e, k).wait_send()
        for k in range(2):
            col_copy(which, cb, k).wait_send()
        for k in range(8):
            tile_copy(which, h, k).wait_send()

    def peer(buf, group, ss, rs, one, arriving=False):
        k, there, _, opposite = one
        own = group[0]
        return pltpu.make_async_remote_copy(
            src_ref=buf.at[own], dst_ref=buf.at[opposite if arriving else own],
            send_sem=ss.at[k], recv_sem=rs.at[k], device_id=there, device_id_type=MESH,
        )

    def arrive(buf, group, ss, rs):
        for one in group[2]:
            peer(buf, group, ss, rs, one, True).wait_recv()

    def start(spec, value):
        spec[0][spec[1][0]] = value
        for one in spec[1][2]:
            peer(*spec, one).start()

    def slots(buf, n):
        total = [buf[j] for j in range(n)]
        while len(total) > 1:
            total = [
                total[j] + total[j + 1] if j + 1 < len(total) else total[j]
                for j in range(0, len(total), 2)
            ]
        return total[0]

    def finish(spec):
        arrive(*spec)
        return slots(spec[0], spec[1][1])

    def settle(spec):
        for one in spec[1][2]:
            peer(*spec, one).wait_send()

    s_z1 = (z1, line, asend.at[0], arecv.at[0])
    s_p1 = (p1, plane, asend.at[1], arecv.at[1])
    s_z2 = (z2, line, asend.at[2], arecv.at[2])
    s_p2 = (p2, plane, asend.at[3], arecv.at[3])
    g_y = (gy_buf, line, gsend.at[1], grecv.at[1])
    g_f = (gf_buf, plane, gsend.at[2], grecv.at[2])

    def pack(columns):
        tile = jnp.zeros((C, L), F32)
        for j, col in enumerate(columns):
            tile = jnp.where(lane == sub + j * C, col, tile)
        return jnp.sum(tile, axis=0, keepdims=True)

    def unpack(row, j):
        return jnp.sum(jnp.where(lane == sub + j * C, row, 0.0), axis=1, keepdims=True)

    def bring(src, e, cb):
        def body(x, cols):
            right, left = cols
            for y in range(Y):
                t = src[pl.ds(x * Y + y, C, stride=X * Y), :]
                e[x + 1, :, (y + 1) * L : (y + 2) * L] = t
                at = x * Y + y
                right = jnp.where(lane == at, pltpu.roll(t, at + 1, 1), right)
                left = jnp.where(lane == at + half, pltpu.roll(t, at + half, 1), left)
            return right, left

        zero = jnp.zeros((C, L), F32)
        right, left = lax.fori_loop(0, X, body, (zero, zero))
        cb[0] = right
        cb[1] = left

    def columns_of(e, cb):
        def body(x, cols):
            right, left = cols
            for y in range(Y):
                t = e[x + 1, :, (y + 1) * L : (y + 2) * L]
                at = x * Y + y
                right = jnp.where(lane == at, pltpu.roll(t, at + 1, 1), right)
                left = jnp.where(lane == at + half, pltpu.roll(t, at + half, 1), left)
            return right, left

        zero = jnp.zeros((C, L), F32)
        right, left = lax.fori_loop(0, X, body, (zero, zero))
        cb[0] = right
        cb[1] = left

    def build(e, h, xp, dx, xs, blocks):
        for yb in blocks:
            dy = -1 if yb == 0 else (1 if yb == Y + 1 else 0)
            ys = Y - 1 if yb == 0 else (0 if yb == Y + 1 else yb - 1)
            slot = (dx + 1) * 3 + dy + 1
            at = xs * Y + ys
            t = e[xp, :, yb * L : (yb + 1) * L]
            before = pltpu.roll(h[slot], lax.rem(L - at, L), 1)
            after = pltpu.roll(h[slot], half - 1 - at, 1)
            low = jnp.where(lane == 0, before, pltpu.roll(t, 1, 1))
            high = jnp.where(lane == L - 1, after, pltpu.roll(t, L - 1, 1))
            for c, v in enumerate((low, t, high)):
                hi, lo = split(v)
                r_ref[xp, c * C : (c + 1) * C, yb * L : (yb + 1) * L] = hi
                r_ref[xp, (3 + c) * C : (4 + c) * C, yb * L : (yb + 1) * L] = lo

    def taps(xp, lo, hi):
        r = r_ref[xp, :, lo:hi]
        return jnp.concatenate([r, r[0 : 3 * C]], axis=0)

    def spread(m_ref, xp, lo, hi, which):
        part = jnp.dot(
            m_ref[which[0] * 3 * C : (which[-1] + 1) * 3 * C, :], taps(xp, lo, hi),
            preferred_element_type=F32,
        )
        for ia, a in enumerate(which):
            for b in range(3):
                row = (ia * 3 + b) * C
                at = lo + (2 - b) * L
                o_ref[xp - a + 2, :, at : at + hi - lo] += part[row : row + C]

    def clear():
        def body(x, carry):
            o_ref[x] = jnp.zeros((C, (Y + 4) * L), F32)
            return carry

        lax.fori_loop(0, X + 4, body, 0)

    def interior(m_ref, e, h):
        def body(x, carry):
            build(e, h, x + 1, 0, x, range(1, Y + 1))
            spread(m_ref, x + 1, I0, I1, (0, 1, 2))
            return carry

        lax.fori_loop(0, X, body, 0)

    def rim(m_ref, e, h):
        build(e, h, 0, -1, X - 1, range(Y + 2))
        spread(m_ref, 0, 0, W, (0,))
        build(e, h, X + 1, 1, 0, range(Y + 2))
        spread(m_ref, X + 1, 0, W, (2,))

        def body(x, carry):
            build(e, h, x + 1, 0, x, (0, Y + 1))
            spread(m_ref, x + 1, 0, L, (0, 1, 2))
            spread(m_ref, x + 1, I1, I1 + L, (0, 1, 2))
            return carry

        lax.fori_loop(0, X, body, 0)

    def clear_pad(ref):
        for x in range(X + 4):
            if x < 2 or x >= X + 2:
                ref[x] = jnp.zeros((2 * C, (Y + 4) * L), BF)
            else:
                ref[x, :, 0 : 2 * L] = jnp.zeros((2 * C, 2 * L), BF)
                ref[x, :, (Y + 2) * L : (Y + 4) * L] = jnp.zeros((2 * C, 2 * L), BF)

    def put_pad(ref, x, v):
        hi, lo = split(v)
        ref[x + 2, 0:C, 2 * L : (Y + 2) * L] = hi
        ref[x + 2, C : 2 * C, 2 * L : (Y + 2) * L] = lo

    def correlate(ref):
        acc_ref[...] = jnp.zeros((2 * ROWS, L), F32)

        def body(xp, carry):
            left = jnp.concatenate(
                [
                    ref[xp - a + 2, :, (2 - b) * L : (2 - b) * L + W]
                    for a in range(3)
                    for b in range(3)
                ],
                axis=0,
            )
            acc_ref[:, 0 : 6 * C] += lax.dot_general(
                left, r_ref[xp], (((1,), (1,)), ((), ())), preferred_element_type=F32
            )
            return carry

        lax.fori_loop(0, X + 2, body, 0)
        pieces = []
        for k in range(9):
            t = acc_ref[2 * k * C : (2 * k + 1) * C] + acc_ref[(2 * k + 1) * C : (2 * k + 2) * C]
            pieces.append(t + pltpu.roll(t, L - 3 * C, 1))
        return pieces

    def put_weights(m_ref, k, t):
        hi = t.astype(BF).astype(F32)
        m_ref[k * C : (k + 1) * C, :] = jnp.concatenate([hi, hi, t - hi], axis=1).astype(BF)

    def weights_forward():
        for k in range(9):
            at = k * 3 * C
            put_weights(
                mf_ref, k,
                jnp.concatenate([wv[at + c * C : at + (c + 1) * C] for c in range(3)], axis=1),
            )

    def weights_backward():
        for k in range(9):
            at = (8 - k) * 3 * C
            put_weights(
                mb_ref, k,
                jnp.concatenate(
                    [wv[at + c * C : at + (c + 1) * C] for c in (2, 1, 0)], axis=0
                ).T,
            )

    def as_column(ref):
        square = lax.broadcasted_iota(jnp.int32, (C, C), 0) == lax.broadcasted_iota(
            jnp.int32, (C, C), 1
        )
        return jnp.sum(jnp.where(square, ref[...], 0.0), axis=1, keepdims=True)

    loads[0].wait()
    bring(vin, ev, cbv)
    pl.semaphore_wait(barrier, greets)
    send_cols(0, cbv)
    send_faces(0, ev)
    for copy in loads[1:]:
        copy.wait()
    clear()
    weights_forward()
    bring(cin, ec, cbc)
    pass_tiles(0, cbv, hv)
    send_cols(1, cbc)
    send_faces(1, ec)
    interior(mf_ref, ev, hv)
    clear_pad(agp)
    clear_pad(cvp)
    weights_backward()

    def vol_sum(x, s):
        return s + jnp.sum(ev[x + 1, :, I0:I1], axis=1, keepdims=True)

    in_sum = lax.fori_loop(0, X, vol_sum, jnp.zeros((C, 1), F32))
    wait_halo(0, ev, hv)
    rim(mf_ref, ev, hv)

    def gather_conv(x, sums):
        s, q = sums
        t = o_ref[x + 2, :, 2 * L : (Y + 2) * L]
        eo[x + 1, :, I0:I1] = t
        return (
            s + jnp.sum(t, axis=1, keepdims=True),
            q + jnp.sum(t * t, axis=1, keepdims=True),
        )

    zero_col = jnp.zeros((C, 1), F32)
    s, q = lax.fori_loop(0, X, gather_conv, (zero_col, zero_col))
    start(s_z1, pack((s, q, in_sum)))
    columns_of(eo, cbo)
    send_cols(2, cbo)

    def pad_conv(x, carry):
        put_pad(cvp, x, eo[x + 1, :, I0:I1])
        return carry

    lax.fori_loop(0, X, pad_conv, 0)
    part = finish(s_z1)
    start(s_p1, part)
    send_faces(2, eo)
    pass_tiles(1, cbc, hc)
    cross = correlate(cvp)
    for k in range(9):
        gw[k * C : (k + 1) * C] = pltpu.roll(cross[k], half, 1)
    pass_tiles(2, cbo, ho)
    clear()
    gain = as_column(gv)
    shift = as_column(bv)
    total1 = finish(s_p1)
    mean = unpack(total1, 0) / count
    var = unpack(total1, 1) / count - mean * mean
    rstd = lax.rsqrt(var + 1e-05)

    def slope(conv, cot):
        normed = (conv - mean) * rstd
        act = gain * normed + shift
        sig = 1.0 / (1.0 + jnp.exp(-act))
        return cot * sig * (1.0 + act * (1.0 - sig)), normed

    def local_slope(x, sums):
        sg, sb = sums
        a, normed = slope(eo[x + 1, :, I0:I1], ec[x + 1, :, I0:I1])
        ea[x + 1, :, I0:I1] = a
        put_pad(agp, x, a)
        return (
            sg + jnp.sum(a * normed, axis=1, keepdims=True),
            sb + jnp.sum(a, axis=1, keepdims=True),
        )

    sg, sb = lax.fori_loop(0, X, local_slope, (zero_col, zero_col))
    start(s_z2, pack((sg, sb)))
    cross = correlate(agp)
    for k in range(9):
        gw[k * C : (k + 1) * C] = jnp.where(lane < half, cross[k], gw[k * C : (k + 1) * C])
    if gw.shape[0] > ROWS:
        gw[ROWS:] = jnp.zeros((gw.shape[0] - ROWS, L), F32)
    chunk = gw.shape[0] // npl

    def piece(j):
        return gw.at[pl.ds(pl.multiple_of(j * chunk, 8), chunk)]

    def scatter(one, arriving=False):
        k, there, to, opposite = one
        return pltpu.make_async_remote_copy(
            src_ref=piece(to), dst_ref=gp_buf.at[opposite if arriving else mp],
            send_sem=gsend.at[0, k], recv_sem=grecv.at[0, k],
            device_id=there, device_id_type=MESH,
        )

    gp_buf[mp] = gw[pl.ds(pl.multiple_of(mp * chunk, 8), chunk)]
    for one in plane[2]:
        scatter(one).start()

    wait_halo(1, ec, hc)
    wait_halo(2, eo, ho)
    for xp in (0, X + 1):
        a, _ = slope(eo[xp], ec[xp])
        ea[xp] = a

    def edge_slope(x, carry):
        for at in (0, I1):
            a, _ = slope(eo[x + 1, :, at : at + L], ec[x + 1, :, at : at + L])
            ea[x + 1, :, at : at + L] = a
        return carry

    lax.fori_loop(0, X, edge_slope, 0)

    def tile_slope(k, carry):
        a, _ = slope(ho[k], hc[k])
        ha[k] = a
        return carry

    lax.fori_loop(0, 9, tile_slope, 0)

    part = finish(s_z2)
    start(s_p2, part)
    for one in plane[2]:
        scatter(one, True).wait_recv()
    start(g_y, slots(gp_buf, npl))
    total2 = finish(s_p2)
    gain_grad = unpack(total2, 0)
    shift_grad = unpack(total2, 1)
    scale = gain * rstd
    k_conv = -scale * rstd * (gain_grad / count)
    k_one = -scale * (shift_grad / count) - k_conv * mean

    def blend(xp, carry):
        ea[xp] = scale * ea[xp] + k_conv * eo[xp] + k_one
        return carry

    lax.fori_loop(0, X + 2, blend, 0)

    def blend_tile(k, carry):
        ha[k] = scale * ha[k] + k_conv * ho[k] + k_one
        return carry

    lax.fori_loop(0, 9, blend_tile, 0)
    interior(mb_ref, ea, ha)
    gpart = finish(g_y)
    start(g_f, gpart)
    rim(mb_ref, ea, ha)

    def emit(x, carry):
        for y in range(Y):
            out_ref[pl.ds(x * Y + y, C, stride=X * Y), :] = o_ref[
                x + 2, :, (y + 2) * L : (y + 3) * L
            ]
        return carry

    lax.fori_loop(0, X, emit, 0)
    gout_ref[...] = total2[:, 0:C]
    bout_ref[...] = pltpu.roll(total2, L - C, 1)[:, 0:C]
    wide = jnp.sum(
        jnp.where(lax.rem(lane, C) == sub, unpack(total1, 2), 0.0), axis=0, keepdims=True
    )
    arrive(*g_f)
    for j in range(npl):
        gfull[j * chunk : (j + 1) * chunk] = gf_buf[j]
    for k in range(9):
        t = gfull[k * C : (k + 1) * C]
        norm = rstd * (pltpu.roll(t, half, 1) - mean * wide)
        t = scale * (t - (shift_grad / count) * wide - (gain_grad / count) * norm)
        for c in range(3):
            at = (k * 3 + c) * C
            wout_ref[at : at + C, :] = (t if c == 0 else pltpu.roll(t, L - c * C, 1))[:, 0:C]

    drain_halo(0, ev, cbv, hv)
    drain_halo(1, ec, cbc, hc)
    drain_halo(2, eo, cbo, ho)
    for spec in (s_z1, s_p1, s_z2, s_p2, g_y, g_f):
        settle(spec)
    for one in plane[2]:
        scatter(one).wait_send()


def store(*refs):
    n = len(refs) // 2
    sem = refs[-1]
    copies = [
        pltpu.make_async_copy(refs[k], refs[n + k], sem.at[k]) for k in range(n)
    ]
    for copy in copies:
        copy.start()
    for copy in copies:
        copy.wait()


def shards(sizes, volume, weight, gamma, beta, cotangent):
    nx, ny, nz = sizes
    _, X, Y, Z = volume.shape
    count = float(X * Y * Z * nx * ny * nz)
    W = (Y + 2) * L
    npl = nx * nz
    chunk = -(-(ROWS // 8) // npl) * 8
    rows = chunk * npl
    vmem = pl.BlockSpec(memory_space=pltpu.VMEM)
    e_shape = pltpu.VMEM((X + 2, C, W), F32)
    h_shape = pltpu.VMEM((9, C, L), F32)
    cb_shape = pltpu.VMEM((4, C, L), F32)
    pad_shape = pltpu.VMEM((X + 4, 2 * C, (Y + 4) * L), BF)
    m_shape = pltpu.VMEM((ROWS, ROWS), BF)
    line_rows = pltpu.VMEM((ny, 1, L), F32)
    plane_rows = pltpu.VMEM((npl, 1, L), F32)
    dma = pltpu.SemaphoreType.DMA
    most = max(npl, ny)
    results = (
        jax.ShapeDtypeStruct((C * X * Y, L), F32),
        jax.ShapeDtypeStruct((27 * C, C), F32),
        jax.ShapeDtypeStruct((1, C), F32),
        jax.ShapeDtypeStruct((1, C), F32),
    )
    made = pl.pallas_call(
        functools.partial(kernel, (nx, ny, nz, X, Y), count),
        out_shape=results,
        in_specs=[pl.BlockSpec(memory_space=pltpu.HBM)] * 5,
        out_specs=(vmem, vmem, vmem, vmem),
        scratch_shapes=[
            pltpu.VMEM((C * X * Y, L), F32), pltpu.VMEM((C * X * Y, L), F32),
            pltpu.VMEM((27 * C, C), F32), pltpu.VMEM((1, C), F32), pltpu.VMEM((1, C), F32),
            m_shape, m_shape,
            e_shape, e_shape, e_shape, e_shape,
            h_shape, h_shape, h_shape, h_shape,
            cb_shape, cb_shape, cb_shape,
            pltpu.VMEM((X + 2, 6 * C, W), BF),
            pltpu.VMEM((X + 4, C, (Y + 4) * L), F32),
            pad_shape, pad_shape,
            pltpu.VMEM((2 * ROWS, L), F32),
            pltpu.VMEM((rows, L), F32), pltpu.VMEM((rows, L), F32),
            line_rows, plane_rows, line_rows, plane_rows,
            pltpu.VMEM((npl, chunk, L), F32), pltpu.VMEM((ny, chunk, L), F32),
            pltpu.VMEM((npl, chunk, L), F32),
            dma((5,)), dma((3, 18)), dma((3, 18)), dma((4, most)), dma((4, most)),
            dma((3, most)), dma((3, most)),
        ],
        compiler_params=pltpu.CompilerParams(
            collective_id=0, has_side_effects=True, vmem_limit_bytes=24 << 20
        ),
    )(
        *(
            pltpu.with_memory_space_constraint(v, pltpu.HBM)
            for v in (
                volume.reshape(C * X * Y, L), cotangent.reshape(C * X * Y, L),
                weight.transpose(2, 3, 4, 0, 1).reshape(27 * C, C),
                gamma.reshape(1, C), beta.reshape(1, C),
            )
        )
    )
    flat, wflat, gain_grad, shift_grad = pl.pallas_call(
        store,
        out_shape=results,
        in_specs=[vmem] * 4,
        out_specs=[pl.BlockSpec(memory_space=pltpu.HBM)] * 4,
        scratch_shapes=[dma((4,))],
        compiler_params=pltpu.CompilerParams(vmem_limit_bytes=8 << 20),
    )(*made)
    return (
        flat.reshape(C, X, Y, Z),
        wflat.reshape(3, 3, 3, C, C).transpose(3, 4, 0, 1, 2),
        gain_grad.reshape(C),
        shift_grad.reshape(C),
    )


def solution(mesh):
    sizes = tuple(mesh.shape[name] for name in ("gx", "gy", "gz"))
    spec = P(None, "gx", "gy", "gz")
    return jax.shard_map(
        functools.partial(shards, sizes),
        mesh=mesh,
        in_specs=(spec, P(), P(), P(), spec),
        out_specs=(spec, P(), P(), P()),
        check_vma=False,
    )
```

```python
import functools

import jax
import jax.numpy as jnp
from jax import lax
from jax.experimental import pallas as pl
from jax.experimental.pallas import tpu as pltpu
from jax.sharding import PartitionSpec as P

MESH = pl.DeviceIdType.MESH
L = 128
C = 16
ROWS = 9 * C
BF = jnp.bfloat16
F32 = jnp.float32
SIDES = [(sx, sy) for sx in (-1, 0, 1) for sy in (-1, 0, 1) if (sx, sy) != (0, 0)]


def split(v):
    hi = v.astype(BF)
    lo = (v - hi.astype(F32)).astype(BF)
    return hi, lo


def kernel(
    dims, count, vol_ref, cot_ref, w_ref, gain_ref, shift_ref,
    out_ref, wout_ref, gout_ref, bout_ref,
    vin, cin, wv, gv, bv, mf_ref, mb_ref, ev, ec, eo, ea, hv, hc, ho, ha, cbv, cbc, cbo,
    r_ref, o_ref, agp, cvp, acc_ref, gw, gfull,
    z1, p1, z2, p2, gp_buf, gy_buf, gf_buf,
    in_sem, hsend, hrecv, asend, arecv, gsend, grecv,
):
    nx, ny, nz, X, Y = dims
    W = (Y + 2) * L
    I0, I1 = L, (Y + 1) * L
    mx, my, mz = lax.axis_index("gx"), lax.axis_index("gy"), lax.axis_index("gz")
    lane = lax.broadcasted_iota(jnp.int32, (C, L), 1)
    sub = lax.broadcasted_iota(jnp.int32, (C, L), 0)
    half = L // 2
    npl = nx * nz
    xs_at = [mx] + [lax.rem(mx + d, nx) for d in range(1, nx)]
    ys_at = [my] + [lax.rem(my + d, ny) for d in range(1, ny)]
    zs_at = [mz] + [lax.rem(mz + d, nz) for d in range(1, nz)]
    xs_row = [x * nz for x in xs_at]
    mp = xs_row[0] + mz
    plane = (
        mp, npl,
        [
            ({"gx": xs_at[dx], "gz": zs_at[dz]}, xs_row[dx] + zs_at[dz])
            for dx in range(nx)
            for dz in range(nz)
            if dx or dz
        ],
    )
    line = (my, ny, [({"gy": ys_at[d]}, ys_at[d]) for d in range(1, ny)])

    def side_id(sx, sy):
        out = {}
        if sx:
            out["gx"] = xs_at[sx]
        if sy:
            out["gy"] = ys_at[sy]
        return out

    loads = [
        pltpu.make_async_copy(src, dst, in_sem.at[k])
        for k, (src, dst) in enumerate(
            ((vol_ref, vin), (cot_ref, cin), (w_ref, wv), (gain_ref, gv), (shift_ref, bv))
        )
    ]
    for copy in loads:
        copy.start()

    barrier = pltpu.get_barrier_semaphore()
    greets = 0
    for group in (plane, line):
        for there, _ in group[2]:
            pl.semaphore_signal(barrier, inc=1, device_id=there, device_id_type=MESH)
            greets += 1
    for sx, sy in SIDES:
        if sx and sy:
            pl.semaphore_signal(barrier, inc=1, device_id=side_id(sx, sy), device_id_type=MESH)
            greets += 1

    def face(ref, sx, sy):
        src_x = {1: X, -1: 1, 0: pl.ds(1, X)}[sx]
        dst_x = {1: 0, -1: X + 1, 0: pl.ds(1, X)}[sx]
        src_y = {1: pl.ds(Y * L, L), -1: pl.ds(L, L), 0: pl.ds(I0, Y * L)}[sy]
        dst_y = {1: pl.ds(0, L), -1: pl.ds(I1, L), 0: pl.ds(I0, Y * L)}[sy]
        return ref.at[src_x, :, src_y], ref.at[dst_x, :, dst_y]

    def await_bytes(ref, sem):
        pltpu.make_async_copy(ref, ref, sem).wait()

    def face_copy(which, ref, k):
        sx, sy = SIDES[k]
        src, dst = face(ref, sx, sy)
        kind = 2 if sx and sy else (0 if sx else 1)
        return pltpu.make_async_remote_copy(
            src_ref=src, dst_ref=dst, send_sem=hsend.at[which, kind], recv_sem=hrecv.at[which, kind],
            device_id=side_id(sx, sy), device_id_type=MESH,
        )

    def col_copy(which, cb, k):
        s = 1 - 2 * k
        return pltpu.make_async_remote_copy(
            src_ref=cb.at[k], dst_ref=cb.at[2 + k],
            send_sem=hsend.at[which, 3], recv_sem=hrecv.at[which, 3],
            device_id={"gz": zs_at[s]}, device_id_type=MESH,
        )

    def tile_copy(which, h, k):
        sx, sy = SIDES[k]
        return pltpu.make_async_remote_copy(
            src_ref=h.at[4], dst_ref=h.at[(1 - sx) * 3 + (1 - sy)],
            send_sem=hsend.at[which, 4], recv_sem=hrecv.at[which, 4],
            device_id=side_id(sx, sy), device_id_type=MESH,
        )

    def send_cols(which, cb):
        for k in range(2):
            col_copy(which, cb, k).start()

    def send_faces(which, e):
        for k in (1, 6, 3, 4, 0, 2, 5, 7):
            face_copy(which, e, k).start()

    def pass_tiles(which, cb, h):
        await_bytes(cb.at[pl.ds(2, 2)], hrecv.at[which, 3])
        h[4] = jnp.where(lane < half, cb[2], cb[3])
        for k in range(8):
            tile_copy(which, h, k).start()

    def faces_done(e, h, sems):
        await_bytes(e.at[pl.ds(0, 2), :, pl.ds(I0, Y * L)], sems.at[0])
        await_bytes(e.at[pl.ds(1, X), :, pl.ds(0, 2 * L)], sems.at[1])
        await_bytes(e.at[0, :, pl.ds(0, 4 * L)], sems.at[2])
        await_bytes(h.at[pl.ds(0, 8)], sems.at[4])

    def wait_halo(which, e, h):
        faces_done(e, h, hrecv.at[which])

    def drain_halo(which, e, cb, h):
        faces_done(e, h, hsend.at[which])
        await_bytes(cb.at[pl.ds(0, 2)], hsend.at[which, 3])

    def peer(buf, group, ss, rs, one):
        there, own = one[0], group[0]
        return pltpu.make_async_remote_copy(
            src_ref=buf.at[own], dst_ref=buf.at[own], send_sem=ss, recv_sem=rs,
            device_id=there, device_id_type=MESH,
        )

    def arrive(buf, group, ss, rs):
        await_bytes(buf.at[pl.ds(0, group[1] - 1)], rs)

    def start(spec, value):
        spec[0][spec[1][0]] = value
        for one in spec[1][2]:
            peer(*spec, one).start()

    def slots(buf, n):
        total = [buf[j] for j in range(n)]
        while len(total) > 1:
            total = [
                total[j] + total[j + 1] if j + 1 < len(total) else total[j]
                for j in range(0, len(total), 2)
            ]
        return total[0]

    def finish(spec):
        arrive(*spec)
        return slots(spec[0], spec[1][1])

    def settle(spec):
        await_bytes(spec[0].at[pl.ds(0, spec[1][1] - 1)], spec[2])

    s_z1 = (z1, line, asend.at[0], arecv.at[0])
    s_p1 = (p1, plane, asend.at[1], arecv.at[1])
    s_z2 = (z2, line, asend.at[2], arecv.at[2])
    s_p2 = (p2, plane, asend.at[3], arecv.at[3])
    g_y = (gy_buf, line, gsend.at[1], grecv.at[1])
    g_f = (gf_buf, plane, gsend.at[2], grecv.at[2])

    def pack(columns):
        tile = jnp.zeros((C, L), F32)
        for j, col in enumerate(columns):
            tile = jnp.where(lane == sub + j * C, col, tile)
        return jnp.sum(tile, axis=0, keepdims=True)

    def unpack(row, j):
        return jnp.sum(jnp.where(lane == sub + j * C, row, 0.0), axis=1, keepdims=True)

    def bring(src, e, cb):
        def body(x, cols):
            right, left = cols
            for y in range(Y):
                t = src[pl.ds(x * Y + y, C, stride=X * Y), :]
                e[x + 1, :, (y + 1) * L : (y + 2) * L] = t
                at = x * Y + y
                right = jnp.where(lane == at, pltpu.roll(t, at + 1, 1), right)
                left = jnp.where(lane == at + half, pltpu.roll(t, at + half, 1), left)
            return right, left

        zero = jnp.zeros((C, L), F32)
        right, left = lax.fori_loop(0, X, body, (zero, zero))
        cb[0] = right
        cb[1] = left

    def columns_of(e, cb):
        def body(x, cols):
            right, left = cols
            for y in range(Y):
                t = e[x + 1, :, (y + 1) * L : (y + 2) * L]
                at = x * Y + y
                right = jnp.where(lane == at, pltpu.roll(t, at + 1, 1), right)
                left = jnp.where(lane == at + half, pltpu.roll(t, at + half, 1), left)
            return right, left

        zero = jnp.zeros((C, L), F32)
        right, left = lax.fori_loop(0, X, body, (zero, zero))
        cb[0] = right
        cb[1] = left

    def build(e, h, xp, dx, xs, blocks):
        for yb in blocks:
            dy = -1 if yb == 0 else (1 if yb == Y + 1 else 0)
            ys = Y - 1 if yb == 0 else (0 if yb == Y + 1 else yb - 1)
            slot = (dx + 1) * 3 + dy + 1
            at = xs * Y + ys
            t = e[xp, :, yb * L : (yb + 1) * L]
            before = pltpu.roll(h[slot], lax.rem(L - at, L), 1)
            after = pltpu.roll(h[slot], half - 1 - at, 1)
            low = jnp.where(lane == 0, before, pltpu.roll(t, 1, 1))
            high = jnp.where(lane == L - 1, after, pltpu.roll(t, L - 1, 1))
            for c, v in enumerate((low, t, high)):
                hi, lo = split(v)
                r_ref[xp, c * C : (c + 1) * C, yb * L : (yb + 1) * L] = hi
                r_ref[xp, (3 + c) * C : (4 + c) * C, yb * L : (yb + 1) * L] = lo

    def taps(xp, lo, hi):
        r = r_ref[xp, :, lo:hi]
        return jnp.concatenate([r, r[0 : 3 * C]], axis=0)

    def spread(m_ref, xp, lo, hi, which):
        part = jnp.dot(
            m_ref[which[0] * 3 * C : (which[-1] + 1) * 3 * C, :], taps(xp, lo, hi),
            preferred_element_type=F32,
        )
        for ia, a in enumerate(which):
            for b in range(3):
                row = (ia * 3 + b) * C
                at = lo + (2 - b) * L
                o_ref[xp - a + 2, :, at : at + hi - lo] += part[row : row + C]

    def clear():
        def body(x, carry):
            o_ref[x] = jnp.zeros((C, (Y + 4) * L), F32)
            return carry

        lax.fori_loop(0, X + 4, body, 0)

    def interior(m_ref, e, h):
        def body(x, carry):
            build(e, h, x + 1, 0, x, range(1, Y + 1))
            spread(m_ref, x + 1, I0, I1, (0, 1, 2))
            return carry

        lax.fori_loop(0, X, body, 0)

    def rim(m_ref, e, h):
        build(e, h, 0, -1, X - 1, range(Y + 2))
        spread(m_ref, 0, 0, W, (0,))
        build(e, h, X + 1, 1, 0, range(Y + 2))
        spread(m_ref, X + 1, 0, W, (2,))

        def body(x, carry):
            build(e, h, x + 1, 0, x, (0, Y + 1))
            spread(m_ref, x + 1, 0, L, (0, 1, 2))
            spread(m_ref, x + 1, I1, I1 + L, (0, 1, 2))
            return carry

        lax.fori_loop(0, X, body, 0)

    def clear_pad(ref):
        for x in range(X + 4):
            if x < 2 or x >= X + 2:
                ref[x] = jnp.zeros((2 * C, (Y + 4) * L), BF)
            else:
                ref[x, :, 0 : 2 * L] = jnp.zeros((2 * C, 2 * L), BF)
                ref[x, :, (Y + 2) * L : (Y + 4) * L] = jnp.zeros((2 * C, 2 * L), BF)

    def put_pad(ref, x, v):
        hi, lo = split(v)
        ref[x + 2, 0:C, 2 * L : (Y + 2) * L] = hi
        ref[x + 2, C : 2 * C, 2 * L : (Y + 2) * L] = lo

    def correlate(ref):
        acc_ref[...] = jnp.zeros((2 * ROWS, L), F32)

        def body(xp, carry):
            left = jnp.concatenate(
                [
                    ref[xp - a + 2, :, (2 - b) * L : (2 - b) * L + W]
                    for a in range(3)
                    for b in range(3)
                ],
                axis=0,
            )
            acc_ref[:, 0 : 6 * C] += lax.dot_general(
                left, r_ref[xp], (((1,), (1,)), ((), ())), preferred_element_type=F32
            )
            return carry

        lax.fori_loop(0, X + 2, body, 0)
        pieces = []
        for k in range(9):
            t = acc_ref[2 * k * C : (2 * k + 1) * C] + acc_ref[(2 * k + 1) * C : (2 * k + 2) * C]
            pieces.append(t + pltpu.roll(t, L - 3 * C, 1))
        return pieces

    def put_weights(m_ref, k, t):
        hi = t.astype(BF).astype(F32)
        m_ref[k * C : (k + 1) * C, :] = jnp.concatenate([hi, hi, t - hi], axis=1).astype(BF)

    def weights_forward():
        for k in range(9):
            at = k * 3 * C
            put_weights(
                mf_ref, k,
                jnp.concatenate([wv[at + c * C : at + (c + 1) * C] for c in range(3)], axis=1),
            )

    def weights_backward():
        for k in range(9):
            at = (8 - k) * 3 * C
            put_weights(
                mb_ref, k,
                jnp.concatenate(
                    [wv[at + c * C : at + (c + 1) * C] for c in (2, 1, 0)], axis=0
                ).T,
            )

    def as_column(ref):
        square = lax.broadcasted_iota(jnp.int32, (C, C), 0) == lax.broadcasted_iota(
            jnp.int32, (C, C), 1
        )
        return jnp.sum(jnp.where(square, ref[...], 0.0), axis=1, keepdims=True)

    loads[0].wait()
    bring(vin, ev, cbv)
    pl.semaphore_wait(barrier, greets)
    send_cols(0, cbv)
    send_faces(0, ev)
    for copy in loads[1:]:
        copy.wait()
    clear()
    weights_forward()
    bring(cin, ec, cbc)
    pass_tiles(0, cbv, hv)
    send_cols(1, cbc)
    send_faces(1, ec)
    interior(mf_ref, ev, hv)
    clear_pad(agp)
    clear_pad(cvp)
    weights_backward()

    def vol_sum(x, s):
        return s + jnp.sum(ev[x + 1, :, I0:I1], axis=1, keepdims=True)

    in_sum = lax.fori_loop(0, X, vol_sum, jnp.zeros((C, 1), F32))
    wait_halo(0, ev, hv)
    rim(mf_ref, ev, hv)

    def gather_conv(x, sums):
        s, q = sums
        t = o_ref[x + 2, :, 2 * L : (Y + 2) * L]
        eo[x + 1, :, I0:I1] = t
        return (
            s + jnp.sum(t, axis=1, keepdims=True),
            q + jnp.sum(t * t, axis=1, keepdims=True),
        )

    zero_col = jnp.zeros((C, 1), F32)
    s, q = lax.fori_loop(0, X, gather_conv, (zero_col, zero_col))
    start(s_z1, pack((s, q, in_sum)))
    columns_of(eo, cbo)
    send_cols(2, cbo)

    def pad_conv(x, carry):
        put_pad(cvp, x, eo[x + 1, :, I0:I1])
        return carry

    lax.fori_loop(0, X, pad_conv, 0)
    part = finish(s_z1)
    start(s_p1, part)
    send_faces(2, eo)
    pass_tiles(1, cbc, hc)
    cross = correlate(cvp)
    for k in range(9):
        gw[k * C : (k + 1) * C] = pltpu.roll(cross[k], half, 1)
    pass_tiles(2, cbo, ho)
    clear()
    gain = as_column(gv)
    shift = as_column(bv)
    total1 = finish(s_p1)
    mean = unpack(total1, 0) / count
    var = unpack(total1, 1) / count - mean * mean
    rstd = lax.rsqrt(var + 1e-05)

    def slope(conv, cot):
        normed = (conv - mean) * rstd
        act = gain * normed + shift
        sig = 1.0 / (1.0 + jnp.exp(-act))
        return cot * sig * (1.0 + act * (1.0 - sig)), normed

    def local_slope(x, sums):
        sg, sb = sums
        a, normed = slope(eo[x + 1, :, I0:I1], ec[x + 1, :, I0:I1])
        ea[x + 1, :, I0:I1] = a
        put_pad(agp, x, a)
        return (
            sg + jnp.sum(a * normed, axis=1, keepdims=True),
            sb + jnp.sum(a, axis=1, keepdims=True),
        )

    sg, sb = lax.fori_loop(0, X, local_slope, (zero_col, zero_col))
    start(s_z2, pack((sg, sb)))
    cross = correlate(agp)
    for k in range(9):
        gw[k * C : (k + 1) * C] = jnp.where(lane < half, cross[k], gw[k * C : (k + 1) * C])
    if gw.shape[0] > ROWS:
        gw[ROWS:] = jnp.zeros((gw.shape[0] - ROWS, L), F32)
    chunk = gw.shape[0] // npl

    def piece(j):
        return gw.at[pl.ds(pl.multiple_of(j * chunk, 8), chunk)]

    def scatter(one):
        there, to = one
        return pltpu.make_async_remote_copy(
            src_ref=piece(to), dst_ref=gp_buf.at[mp], send_sem=gsend.at[0], recv_sem=grecv.at[0],
            device_id=there, device_id_type=MESH,
        )

    gp_buf[mp] = gw[pl.ds(pl.multiple_of(mp * chunk, 8), chunk)]
    for one in plane[2]:
        scatter(one).start()

    wait_halo(1, ec, hc)
    wait_halo(2, eo, ho)
    for xp in (0, X + 1):
        a, _ = slope(eo[xp], ec[xp])
        ea[xp] = a

    def edge_slope(x, carry):
        for at in (0, I1):
            a, _ = slope(eo[x + 1, :, at : at + L], ec[x + 1, :, at : at + L])
            ea[x + 1, :, at : at + L] = a
        return carry

    lax.fori_loop(0, X, edge_slope, 0)

    def tile_slope(k, carry):
        a, _ = slope(ho[k], hc[k])
        ha[k] = a
        return carry

    lax.fori_loop(0, 9, tile_slope, 0)

    part = finish(s_z2)
    start(s_p2, part)
    await_bytes(gp_buf.at[pl.ds(0, npl - 1)], grecv.at[0])
    start(g_y, slots(gp_buf, npl))
    total2 = finish(s_p2)
    gain_grad = unpack(total2, 0)
    shift_grad = unpack(total2, 1)
    scale = gain * rstd
    k_conv = -scale * rstd * (gain_grad / count)
    k_one = -scale * (shift_grad / count) - k_conv * mean

    def blend(xp, carry):
        ea[xp] = scale * ea[xp] + k_conv * eo[xp] + k_one
        return carry

    lax.fori_loop(0, X + 2, blend, 0)

    def blend_tile(k, carry):
        ha[k] = scale * ha[k] + k_conv * ho[k] + k_one
        return carry

    lax.fori_loop(0, 9, blend_tile, 0)
    interior(mb_ref, ea, ha)
    gpart = finish(g_y)
    start(g_f, gpart)
    rim(mb_ref, ea, ha)

    def emit(x, carry):
        for y in range(Y):
            out_ref[pl.ds(x * Y + y, C, stride=X * Y), :] = o_ref[
                x + 2, :, (y + 2) * L : (y + 3) * L
            ]
        return carry

    lax.fori_loop(0, X, emit, 0)
    gout_ref[...] = total2[:, 0:C]
    bout_ref[...] = pltpu.roll(total2, L - C, 1)[:, 0:C]
    wide = jnp.sum(
        jnp.where(lax.rem(lane, C) == sub, unpack(total1, 2), 0.0), axis=0, keepdims=True
    )
    k_norm = scale * rstd * (gain_grad / count)
    k_wide = (k_norm * mean - scale * (shift_grad / count)) * wide
    drain_halo(0, ev, cbv, hv)
    drain_halo(1, ec, cbc, hc)
    drain_halo(2, eo, cbo, ho)
    for spec in (s_z1, s_p1, s_z2, s_p2, g_y):
        settle(spec)
    await_bytes(gp_buf.at[pl.ds(0, npl - 1)], gsend.at[0])
    arrive(*g_f)
    if chunk != 8:
        for j in range(npl):
            gfull[j * chunk : (j + 1) * chunk] = gf_buf[j]
    for k in range(9):
        if chunk == 8:
            t = jnp.concatenate([gf_buf[2 * k], gf_buf[2 * k + 1]], axis=0)
        else:
            t = gfull[k * C : (k + 1) * C]
        t = scale * t - k_norm * pltpu.roll(t, half, 1) + k_wide
        for c in range(3):
            at = (k * 3 + c) * C
            wout_ref[at : at + C, :] = (t if c == 0 else pltpu.roll(t, L - c * C, 1))[:, 0:C]
    settle(g_f)


def store(*refs):
    n = len(refs) // 2
    sem = refs[-1]
    copies = [
        pltpu.make_async_copy(refs[k], refs[n + k], sem.at[k]) for k in range(n)
    ]
    for copy in copies:
        copy.start()
    for copy in copies:
        copy.wait()


def shards(sizes, volume, weight, gamma, beta, cotangent):
    nx, ny, nz = sizes
    _, X, Y, Z = volume.shape
    count = float(X * Y * Z * nx * ny * nz)
    W = (Y + 2) * L
    npl = nx * nz
    chunk = -(-(ROWS // 8) // npl) * 8
    rows = chunk * npl
    vmem = pl.BlockSpec(memory_space=pltpu.VMEM)
    e_shape = pltpu.VMEM((X + 2, C, W), F32)
    h_shape = pltpu.VMEM((9, C, L), F32)
    cb_shape = pltpu.VMEM((4, C, L), F32)
    pad_shape = pltpu.VMEM((X + 4, 2 * C, (Y + 4) * L), BF)
    m_shape = pltpu.VMEM((ROWS, ROWS), BF)
    line_rows = pltpu.VMEM((ny, 1, L), F32)
    plane_rows = pltpu.VMEM((npl, 1, L), F32)
    dma = pltpu.SemaphoreType.DMA
    results = (
        jax.ShapeDtypeStruct((C * X * Y, L), F32),
        jax.ShapeDtypeStruct((27 * C, C), F32),
        jax.ShapeDtypeStruct((1, C), F32),
        jax.ShapeDtypeStruct((1, C), F32),
    )
    made = pl.pallas_call(
        functools.partial(kernel, (nx, ny, nz, X, Y), count),
        out_shape=results,
        in_specs=[pl.BlockSpec(memory_space=pltpu.HBM)] * 5,
        out_specs=(vmem, vmem, vmem, vmem),
        scratch_shapes=[
            pltpu.VMEM((C * X * Y, L), F32), pltpu.VMEM((C * X * Y, L), F32),
            pltpu.VMEM((27 * C, C), F32), pltpu.VMEM((1, C), F32), pltpu.VMEM((1, C), F32),
            m_shape, m_shape,
            e_shape, e_shape, e_shape, e_shape,
            h_shape, h_shape, h_shape, h_shape,
            cb_shape, cb_shape, cb_shape,
            pltpu.VMEM((X + 2, 6 * C, W), BF),
            pltpu.VMEM((X + 4, C, (Y + 4) * L), F32),
            pad_shape, pad_shape,
            pltpu.VMEM((2 * ROWS, L), F32),
            pltpu.VMEM((rows, L), F32), pltpu.VMEM((rows, L), F32),
            line_rows, plane_rows, line_rows, plane_rows,
            pltpu.VMEM((npl, chunk, L), F32), pltpu.VMEM((ny, chunk, L), F32),
            pltpu.VMEM((npl, chunk, L), F32),
            dma((5,)), dma((3, 5)), dma((3, 5)), dma((4,)), dma((4,)), dma((3,)), dma((3,)),
        ],
        compiler_params=pltpu.CompilerParams(
            collective_id=0, has_side_effects=True, vmem_limit_bytes=24 << 20
        ),
    )(
        *(
            pltpu.with_memory_space_constraint(v, pltpu.HBM)
            for v in (
                volume.reshape(C * X * Y, L), cotangent.reshape(C * X * Y, L),
                weight.transpose(2, 3, 4, 0, 1).reshape(27 * C, C),
                gamma.reshape(1, C), beta.reshape(1, C),
            )
        )
    )
    flat, wflat, gain_grad, shift_grad = pl.pallas_call(
        store,
        out_shape=results,
        in_specs=[vmem] * 4,
        out_specs=[pl.BlockSpec(memory_space=pltpu.HBM)] * 4,
        scratch_shapes=[dma((4,))],
        compiler_params=pltpu.CompilerParams(vmem_limit_bytes=8 << 20),
    )(*made)
    return (
        flat.reshape(C, X, Y, Z),
        wflat.reshape(3, 3, 3, C, C).transpose(3, 4, 0, 1, 2),
        gain_grad.reshape(C),
        shift_grad.reshape(C),
    )


def solution(mesh):
    sizes = tuple(mesh.shape[name] for name in ("gx", "gy", "gz"))
    spec = P(None, "gx", "gy", "gz")
    return jax.shard_map(
        functools.partial(shards, sizes),
        mesh=mesh,
        in_specs=(spec, P(), P(), P(), spec),
        out_specs=(spec, P(), P(), P()),
        check_vma=False,
    )
```

```python
import functools

import jax
import jax.numpy as jnp
from jax import lax
from jax.experimental import pallas as pl
from jax.experimental.pallas import tpu as pltpu
from jax.sharding import PartitionSpec as P

MESH = pl.DeviceIdType.MESH
L = 128
C = 16
ROWS = 9 * C
BF = jnp.bfloat16
F32 = jnp.float32
SIDES = [(sx, sy) for sx in (-1, 0, 1) for sy in (-1, 0, 1) if (sx, sy) != (0, 0)]


def split(v):
    hi = v.astype(BF)
    lo = (v - hi.astype(F32)).astype(BF)
    return hi, lo


def kernel(
    dims, count, vol_ref, cot_ref, w_ref, gain_ref, shift_ref,
    out_ref, wout_ref, gout_ref, bout_ref,
    vin, cin, wv, gv, bv, mf_ref, mb_ref, ev, ec, eo, ea, hv, hc, ho, ha, cbv, cbc, cbo,
    r_ref, o_ref, agp, cvp, acc_ref, gw, gfull,
    z1, p1, z2, p2, gp_buf, gy_buf, gf_buf,
    in_sem, hsend, hrecv, asend, arecv, gsend, grecv,
):
    nx, ny, nz, X, Y = dims
    W = (Y + 2) * L
    I0, I1 = L, (Y + 1) * L
    mx, my, mz = lax.axis_index("gx"), lax.axis_index("gy"), lax.axis_index("gz")
    lane = lax.broadcasted_iota(jnp.int32, (C, L), 1)
    sub = lax.broadcasted_iota(jnp.int32, (C, L), 0)
    half = L // 2
    npl = nx * nz
    xs_at = [mx] + [lax.rem(mx + d, nx) for d in range(1, nx)]
    ys_at = [my] + [lax.rem(my + d, ny) for d in range(1, ny)]
    zs_at = [mz] + [lax.rem(mz + d, nz) for d in range(1, nz)]
    xs_row = [x * nz for x in xs_at]
    mp = xs_row[0] + mz
    plane = (
        mp, npl,
        [
            ({"gx": xs_at[dx], "gz": zs_at[dz]}, xs_row[dx] + zs_at[dz])
            for dx in range(nx)
            for dz in range(nz)
            if dx or dz
        ],
    )
    line = (my, ny, [({"gy": ys_at[d]}, ys_at[d]) for d in range(1, ny)])

    def side_id(sx, sy):
        out = {}
        if sx:
            out["gx"] = xs_at[sx]
        if sy:
            out["gy"] = ys_at[sy]
        return out

    loads = [
        pltpu.make_async_copy(src, dst, in_sem.at[k])
        for k, (src, dst) in enumerate(
            ((vol_ref, vin), (cot_ref, cin), (w_ref, wv), (gain_ref, gv), (shift_ref, bv))
        )
    ]
    for copy in loads:
        copy.start()

    barrier = pltpu.get_barrier_semaphore()
    greets = 0
    for group in (plane, line):
        for there, _ in group[2]:
            pl.semaphore_signal(barrier, inc=1, device_id=there, device_id_type=MESH)
            greets += 1
    for sx, sy in SIDES:
        if sx and sy:
            pl.semaphore_signal(barrier, inc=1, device_id=side_id(sx, sy), device_id_type=MESH)
            greets += 1

    def face(ref, sx, sy):
        src_x = {1: X, -1: 1, 0: pl.ds(1, X)}[sx]
        dst_x = {1: 0, -1: X + 1, 0: pl.ds(1, X)}[sx]
        src_y = {1: pl.ds(Y * L, L), -1: pl.ds(L, L), 0: pl.ds(I0, Y * L)}[sy]
        dst_y = {1: pl.ds(0, L), -1: pl.ds(I1, L), 0: pl.ds(I0, Y * L)}[sy]
        return ref.at[src_x, :, src_y], ref.at[dst_x, :, dst_y]

    def await_bytes(ref, sem):
        pltpu.make_async_copy(ref, ref, sem).wait()

    def face_copy(which, ref, k):
        sx, sy = SIDES[k]
        src, dst = face(ref, sx, sy)
        kind = 2 if sx and sy else (0 if sx else 1)
        return pltpu.make_async_remote_copy(
            src_ref=src, dst_ref=dst, send_sem=hsend.at[which, kind], recv_sem=hrecv.at[which, kind],
            device_id=side_id(sx, sy), device_id_type=MESH,
        )

    def col_copy(which, cb, k):
        s = 1 - 2 * k
        return pltpu.make_async_remote_copy(
            src_ref=cb.at[k], dst_ref=cb.at[2 + k],
            send_sem=hsend.at[which, 3], recv_sem=hrecv.at[which, 3],
            device_id={"gz": zs_at[s]}, device_id_type=MESH,
        )

    def tile_copy(which, h, k):
        sx, sy = SIDES[k]
        kind = 4 if sx else 5
        return pltpu.make_async_remote_copy(
            src_ref=h.at[4], dst_ref=h.at[(1 - sx) * 3 + (1 - sy)],
            send_sem=hsend.at[which, kind], recv_sem=hrecv.at[which, kind],
            device_id=side_id(sx, sy), device_id_type=MESH,
        )

    def send_cols(which, cb):
        for k in range(2):
            col_copy(which, cb, k).start()

    def send_faces(which, e):
        for k in (1, 6, 3, 4, 0, 2, 5, 7):
            face_copy(which, e, k).start()

    def pass_tiles(which, cb, h):
        await_bytes(cb.at[pl.ds(2, 2)], hrecv.at[which, 3])
        h[4] = jnp.where(lane < half, cb[2], cb[3])
        for k in range(8):
            tile_copy(which, h, k).start()

    def edges_done(e, h, sems):
        await_bytes(e.at[pl.ds(1, X), :, pl.ds(0, 2 * L)], sems.at[1])
        await_bytes(h.at[pl.ds(0, 2)], sems.at[5])

    def sides_done(e, h, sems):
        await_bytes(e.at[pl.ds(0, 2), :, pl.ds(I0, Y * L)], sems.at[0])
        await_bytes(e.at[0, :, pl.ds(0, 4 * L)], sems.at[2])
        await_bytes(h.at[pl.ds(0, 6)], sems.at[4])

    def wait_edges(which, e, h):
        edges_done(e, h, hrecv.at[which])

    def wait_sides(which, e, h):
        sides_done(e, h, hrecv.at[which])

    def wait_halo(which, e, h):
        wait_edges(which, e, h)
        wait_sides(which, e, h)

    def drain_halo(which, e, cb, h):
        edges_done(e, h, hsend.at[which])
        sides_done(e, h, hsend.at[which])
        await_bytes(cb.at[pl.ds(0, 2)], hsend.at[which, 3])

    def peer(buf, group, ss, rs, one):
        there, own = one[0], group[0]
        return pltpu.make_async_remote_copy(
            src_ref=buf.at[own], dst_ref=buf.at[own], send_sem=ss, recv_sem=rs,
            device_id=there, device_id_type=MESH,
        )

    def arrive(buf, group, ss, rs):
        await_bytes(buf.at[pl.ds(0, group[1] - 1)], rs)

    def start(spec, value):
        spec[0][spec[1][0]] = value
        for one in spec[1][2]:
            peer(*spec, one).start()

    def slots(buf, n):
        total = [buf[j] for j in range(n)]
        while len(total) > 1:
            total = [
                total[j] + total[j + 1] if j + 1 < len(total) else total[j]
                for j in range(0, len(total), 2)
            ]
        return total[0]

    def finish(spec):
        arrive(*spec)
        return slots(spec[0], spec[1][1])

    def settle(spec):
        await_bytes(spec[0].at[pl.ds(0, spec[1][1] - 1)], spec[2])

    s_z1 = (z1, line, asend.at[0], arecv.at[0])
    s_p1 = (p1, plane, asend.at[1], arecv.at[1])
    s_z2 = (z2, line, asend.at[2], arecv.at[2])
    s_p2 = (p2, plane, asend.at[3], arecv.at[3])
    g_y = (gy_buf, line, gsend.at[1], grecv.at[1])
    g_f = (gf_buf, plane, gsend.at[2], grecv.at[2])

    def pack(columns):
        tile = jnp.zeros((C, L), F32)
        for j, col in enumerate(columns):
            tile = jnp.where(lane == sub + j * C, col, tile)
        return jnp.sum(tile, axis=0, keepdims=True)

    def unpack(row, j):
        return jnp.sum(jnp.where(lane == sub + j * C, row, 0.0), axis=1, keepdims=True)

    def bring(src, e, cb):
        def body(x, cols):
            right, left = cols
            for y in range(Y):
                t = src[pl.ds(x * Y + y, C, stride=X * Y), :]
                e[x + 1, :, (y + 1) * L : (y + 2) * L] = t
                at = x * Y + y
                right = jnp.where(lane == at, pltpu.roll(t, at + 1, 1), right)
                left = jnp.where(lane == at + half, pltpu.roll(t, at + half, 1), left)
            return right, left

        zero = jnp.zeros((C, L), F32)
        right, left = lax.fori_loop(0, X, body, (zero, zero))
        cb[0] = right
        cb[1] = left

    def columns_of(e, cb):
        def body(x, cols):
            right, left = cols
            for y in range(Y):
                t = e[x + 1, :, (y + 1) * L : (y + 2) * L]
                at = x * Y + y
                right = jnp.where(lane == at, pltpu.roll(t, at + 1, 1), right)
                left = jnp.where(lane == at + half, pltpu.roll(t, at + half, 1), left)
            return right, left

        zero = jnp.zeros((C, L), F32)
        right, left = lax.fori_loop(0, X, body, (zero, zero))
        cb[0] = right
        cb[1] = left

    def build(e, h, xp, dx, xs, blocks):
        for yb in blocks:
            dy = -1 if yb == 0 else (1 if yb == Y + 1 else 0)
            ys = Y - 1 if yb == 0 else (0 if yb == Y + 1 else yb - 1)
            slot = (dx + 1) * 3 + dy + 1
            at = xs * Y + ys
            t = e[xp, :, yb * L : (yb + 1) * L]
            before = pltpu.roll(h[slot], lax.rem(L - at, L), 1)
            after = pltpu.roll(h[slot], half - 1 - at, 1)
            low = jnp.where(lane == 0, before, pltpu.roll(t, 1, 1))
            high = jnp.where(lane == L - 1, after, pltpu.roll(t, L - 1, 1))
            for c, v in enumerate((low, t, high)):
                hi, lo = split(v)
                r_ref[xp, c * C : (c + 1) * C, yb * L : (yb + 1) * L] = hi
                r_ref[xp, (3 + c) * C : (4 + c) * C, yb * L : (yb + 1) * L] = lo

    def taps(xp, lo, hi):
        r = r_ref[xp, :, lo:hi]
        return jnp.concatenate([r, r[0 : 3 * C]], axis=0)

    def spread(m_ref, xp, lo, hi, which):
        part = jnp.dot(
            m_ref[which[0] * 3 * C : (which[-1] + 1) * 3 * C, :], taps(xp, lo, hi),
            preferred_element_type=F32,
        )
        for ia, a in enumerate(which):
            for b in range(3):
                row = (ia * 3 + b) * C
                at = lo + (2 - b) * L
                o_ref[xp - a + 2, :, at : at + hi - lo] += part[row : row + C]

    def clear():
        def body(x, carry):
            o_ref[x] = jnp.zeros((C, (Y + 4) * L), F32)
            return carry

        lax.fori_loop(0, X + 4, body, 0)

    def interior(m_ref, e, h):
        def body(x, carry):
            build(e, h, x + 1, 0, x, range(1, Y + 1))
            spread(m_ref, x + 1, I0, I1, (0, 1, 2))
            return carry

        lax.fori_loop(0, X, body, 0)

    def edges(m_ref, e, h):
        def body(x, carry):
            build(e, h, x + 1, 0, x, (0, Y + 1))
            spread(m_ref, x + 1, 0, L, (0, 1, 2))
            spread(m_ref, x + 1, I1, I1 + L, (0, 1, 2))
            return carry

        lax.fori_loop(0, X, body, 0)

    def rim(m_ref, e, h):
        build(e, h, 0, -1, X - 1, range(Y + 2))
        spread(m_ref, 0, 0, W, (0,))
        build(e, h, X + 1, 1, 0, range(Y + 2))
        spread(m_ref, X + 1, 0, W, (2,))

    def clear_pad(ref):
        for x in range(X):
            ref[x, :, 0 : 2 * L] = jnp.zeros((2 * C, 2 * L), BF)
            ref[x, :, (Y + 2) * L : (Y + 4) * L] = jnp.zeros((2 * C, 2 * L), BF)

    def put_pad(ref, x, v):
        hi, lo = split(v)
        ref[x, 0:C, 2 * L : (Y + 2) * L] = hi
        ref[x, C : 2 * C, 2 * L : (Y + 2) * L] = lo

    def correlate(ref):
        acc_ref[...] = jnp.zeros((2 * ROWS, L), F32)
        for xp in range(X + 2):
            valid = [a for a in range(3) if 0 <= xp - a < X]
            left = jnp.concatenate(
                [
                    ref[xp - a, :, (2 - b) * L : (2 - b) * L + W]
                    for a in valid
                    for b in range(3)
                ],
                axis=0,
            )
            at = valid[0] * 6 * C
            acc_ref[at : at + left.shape[0], 0 : 6 * C] += lax.dot_general(
                left, r_ref[xp], (((1,), (1,)), ((), ())), preferred_element_type=F32
            )
        pieces = []
        for k in range(9):
            t = acc_ref[2 * k * C : (2 * k + 1) * C] + acc_ref[(2 * k + 1) * C : (2 * k + 2) * C]
            pieces.append(t + pltpu.roll(t, L - 3 * C, 1))
        return pieces

    def put_weights(m_ref, k, t):
        hi = t.astype(BF).astype(F32)
        m_ref[k * C : (k + 1) * C, :] = jnp.concatenate([hi, hi, t - hi], axis=1).astype(BF)

    def weights_forward():
        for k in range(9):
            at = k * 3 * C
            put_weights(
                mf_ref, k,
                jnp.concatenate([wv[at + c * C : at + (c + 1) * C] for c in range(3)], axis=1),
            )

    def weights_backward():
        for k in range(9):
            at = (8 - k) * 3 * C
            put_weights(
                mb_ref, k,
                jnp.concatenate(
                    [wv[at + c * C : at + (c + 1) * C] for c in (2, 1, 0)], axis=0
                ).T,
            )

    def as_column(ref):
        square = lax.broadcasted_iota(jnp.int32, (C, C), 0) == lax.broadcasted_iota(
            jnp.int32, (C, C), 1
        )
        return jnp.sum(jnp.where(square, ref[...], 0.0), axis=1, keepdims=True)

    loads[0].wait()
    bring(vin, ev, cbv)
    pl.semaphore_wait(barrier, greets)
    send_cols(0, cbv)
    send_faces(0, ev)
    for copy in loads[1:]:
        copy.wait()
    clear()
    weights_forward()
    bring(cin, ec, cbc)
    pass_tiles(0, cbv, hv)
    send_cols(1, cbc)
    interior(mf_ref, ev, hv)
    clear_pad(agp)
    clear_pad(cvp)
    weights_backward()

    def vol_sum(x, s):
        return s + jnp.sum(ev[x + 1, :, I0:I1], axis=1, keepdims=True)

    in_sum = lax.fori_loop(0, X, vol_sum, jnp.zeros((C, 1), F32))
    wait_edges(0, ev, hv)
    edges(mf_ref, ev, hv)
    wait_sides(0, ev, hv)
    send_faces(1, ec)
    rim(mf_ref, ev, hv)

    def gather_conv(x, sums):
        s, q = sums
        t = o_ref[x + 2, :, 2 * L : (Y + 2) * L]
        eo[x + 1, :, I0:I1] = t
        return (
            s + jnp.sum(t, axis=1, keepdims=True),
            q + jnp.sum(t * t, axis=1, keepdims=True),
        )

    zero_col = jnp.zeros((C, 1), F32)
    s, q = lax.fori_loop(0, X, gather_conv, (zero_col, zero_col))
    start(s_z1, pack((s, q, in_sum)))
    columns_of(eo, cbo)
    send_cols(2, cbo)

    def pad_conv(x, carry):
        put_pad(cvp, x, eo[x + 1, :, I0:I1])
        return carry

    lax.fori_loop(0, X, pad_conv, 0)
    part = finish(s_z1)
    start(s_p1, part)
    send_faces(2, eo)
    pass_tiles(1, cbc, hc)
    cross = correlate(cvp)
    for k in range(9):
        gw[k * C : (k + 1) * C] = pltpu.roll(cross[k], half, 1)
    pass_tiles(2, cbo, ho)
    clear()
    gain = as_column(gv)
    shift = as_column(bv)
    total1 = finish(s_p1)
    mean = unpack(total1, 0) / count
    var = unpack(total1, 1) / count - mean * mean
    rstd = lax.rsqrt(var + 1e-05)

    def slope(conv, cot):
        normed = (conv - mean) * rstd
        act = gain * normed + shift
        sig = 1.0 / (1.0 + jnp.exp(-act))
        return cot * sig * (1.0 + act * (1.0 - sig)), normed

    def local_slope(x, sums):
        sg, sb = sums
        a, normed = slope(eo[x + 1, :, I0:I1], ec[x + 1, :, I0:I1])
        ea[x + 1, :, I0:I1] = a
        put_pad(agp, x, a)
        return (
            sg + jnp.sum(a * normed, axis=1, keepdims=True),
            sb + jnp.sum(a, axis=1, keepdims=True),
        )

    sg, sb = lax.fori_loop(0, X, local_slope, (zero_col, zero_col))
    start(s_z2, pack((sg, sb)))
    cross = correlate(agp)
    for k in range(9):
        gw[k * C : (k + 1) * C] = jnp.where(lane < half, cross[k], gw[k * C : (k + 1) * C])
    if gw.shape[0] > ROWS:
        gw[ROWS:] = jnp.zeros((gw.shape[0] - ROWS, L), F32)
    chunk = gw.shape[0] // npl

    def piece(j):
        return gw.at[pl.ds(pl.multiple_of(j * chunk, 8), chunk)]

    def scatter(one):
        there, to = one
        return pltpu.make_async_remote_copy(
            src_ref=piece(to), dst_ref=gp_buf.at[mp], send_sem=gsend.at[0], recv_sem=grecv.at[0],
            device_id=there, device_id_type=MESH,
        )

    gp_buf[mp] = gw[pl.ds(pl.multiple_of(mp * chunk, 8), chunk)]
    for one in plane[2]:
        scatter(one).start()

    wait_halo(1, ec, hc)
    wait_halo(2, eo, ho)
    for xp in (0, X + 1):
        a, _ = slope(eo[xp], ec[xp])
        ea[xp] = a

    def edge_slope(x, carry):
        for at in (0, I1):
            a, _ = slope(eo[x + 1, :, at : at + L], ec[x + 1, :, at : at + L])
            ea[x + 1, :, at : at + L] = a
        return carry

    lax.fori_loop(0, X, edge_slope, 0)

    def tile_slope(k, carry):
        a, _ = slope(ho[k], hc[k])
        ha[k] = a
        return carry

    lax.fori_loop(0, 9, tile_slope, 0)

    part = finish(s_z2)
    start(s_p2, part)
    await_bytes(gp_buf.at[pl.ds(0, npl - 1)], grecv.at[0])
    start(g_y, slots(gp_buf, npl))
    total2 = finish(s_p2)
    gain_grad = unpack(total2, 0)
    shift_grad = unpack(total2, 1)
    scale = gain * rstd
    k_conv = -scale * rstd * (gain_grad / count)
    k_one = -scale * (shift_grad / count) - k_conv * mean

    def blend(xp, carry):
        ea[xp] = scale * ea[xp] + k_conv * eo[xp] + k_one
        return carry

    lax.fori_loop(0, X + 2, blend, 0)

    def blend_tile(k, carry):
        ha[k] = scale * ha[k] + k_conv * ho[k] + k_one
        return carry

    lax.fori_loop(0, 9, blend_tile, 0)
    interior(mb_ref, ea, ha)
    gpart = finish(g_y)
    start(g_f, gpart)
    edges(mb_ref, ea, ha)
    rim(mb_ref, ea, ha)

    def emit(x, carry):
        for y in range(Y):
            out_ref[pl.ds(x * Y + y, C, stride=X * Y), :] = o_ref[
                x + 2, :, (y + 2) * L : (y + 3) * L
            ]
        return carry

    lax.fori_loop(0, X, emit, 0)
    gout_ref[...] = total2[:, 0:C]
    bout_ref[...] = pltpu.roll(total2, L - C, 1)[:, 0:C]
    wide = jnp.sum(
        jnp.where(lax.rem(lane, C) == sub, unpack(total1, 2), 0.0), axis=0, keepdims=True
    )
    k_norm = scale * rstd * (gain_grad / count)
    k_wide = (k_norm * mean - scale * (shift_grad / count)) * wide
    drain_halo(0, ev, cbv, hv)
    drain_halo(1, ec, cbc, hc)
    drain_halo(2, eo, cbo, ho)
    for spec in (s_z1, s_p1, s_z2, s_p2, g_y):
        settle(spec)
    await_bytes(gp_buf.at[pl.ds(0, npl - 1)], gsend.at[0])
    arrive(*g_f)
    if chunk != 8:
        for j in range(npl):
            gfull[j * chunk : (j + 1) * chunk] = gf_buf[j]
    for k in range(9):
        if chunk == 8:
            t = jnp.concatenate([gf_buf[2 * k], gf_buf[2 * k + 1]], axis=0)
        else:
            t = gfull[k * C : (k + 1) * C]
        t = scale * t - k_norm * pltpu.roll(t, half, 1) + k_wide
        for c in range(3):
            at = (k * 3 + c) * C
            wout_ref[at : at + C, :] = (t if c == 0 else pltpu.roll(t, L - c * C, 1))[:, 0:C]
    settle(g_f)


def store(*refs):
    n = len(refs) // 2
    sem = refs[-1]
    copies = [
        pltpu.make_async_copy(refs[k], refs[n + k], sem.at[k]) for k in range(n)
    ]
    for copy in copies:
        copy.start()
    for copy in copies:
        copy.wait()


def shards(sizes, volume, weight, gamma, beta, cotangent):
    nx, ny, nz = sizes
    _, X, Y, Z = volume.shape
    count = float(X * Y * Z * nx * ny * nz)
    W = (Y + 2) * L
    npl = nx * nz
    chunk = -(-(ROWS // 8) // npl) * 8
    rows = chunk * npl
    vmem = pl.BlockSpec(memory_space=pltpu.VMEM)
    e_shape = pltpu.VMEM((X + 2, C, W), F32)
    h_shape = pltpu.VMEM((9, C, L), F32)
    cb_shape = pltpu.VMEM((4, C, L), F32)
    pad_shape = pltpu.VMEM((X, 2 * C, (Y + 4) * L), BF)
    m_shape = pltpu.VMEM((ROWS, ROWS), BF)
    line_rows = pltpu.VMEM((ny, 1, L), F32)
    plane_rows = pltpu.VMEM((npl, 1, L), F32)
    dma = pltpu.SemaphoreType.DMA
    results = (
        jax.ShapeDtypeStruct((C * X * Y, L), F32),
        jax.ShapeDtypeStruct((27 * C, C), F32),
        jax.ShapeDtypeStruct((1, C), F32),
        jax.ShapeDtypeStruct((1, C), F32),
    )
    made = pl.pallas_call(
        functools.partial(kernel, (nx, ny, nz, X, Y), count),
        out_shape=results,
        in_specs=[pl.BlockSpec(memory_space=pltpu.HBM)] * 5,
        out_specs=(vmem, vmem, vmem, vmem),
        scratch_shapes=[
            pltpu.VMEM((C * X * Y, L), F32), pltpu.VMEM((C * X * Y, L), F32),
            pltpu.VMEM((27 * C, C), F32), pltpu.VMEM((1, C), F32), pltpu.VMEM((1, C), F32),
            m_shape, m_shape,
            e_shape, e_shape, e_shape, e_shape,
            h_shape, h_shape, h_shape, h_shape,
            cb_shape, cb_shape, cb_shape,
            pltpu.VMEM((X + 2, 6 * C, W), BF),
            pltpu.VMEM((X + 4, C, (Y + 4) * L), F32),
            pad_shape, pad_shape,
            pltpu.VMEM((2 * ROWS, L), F32),
            pltpu.VMEM((rows, L), F32), pltpu.VMEM((rows, L), F32),
            line_rows, plane_rows, line_rows, plane_rows,
            pltpu.VMEM((npl, chunk, L), F32), pltpu.VMEM((ny, chunk, L), F32),
            pltpu.VMEM((npl, chunk, L), F32),
            dma((5,)), dma((3, 6)), dma((3, 6)), dma((4,)), dma((4,)), dma((3,)), dma((3,)),
        ],
        compiler_params=pltpu.CompilerParams(
            collective_id=0, has_side_effects=True, vmem_limit_bytes=24 << 20
        ),
    )(
        *(
            pltpu.with_memory_space_constraint(v, pltpu.HBM)
            for v in (
                volume.reshape(C * X * Y, L), cotangent.reshape(C * X * Y, L),
                weight.transpose(2, 3, 4, 0, 1).reshape(27 * C, C),
                gamma.reshape(1, C), beta.reshape(1, C),
            )
        )
    )
    flat, wflat, gain_grad, shift_grad = pl.pallas_call(
        store,
        out_shape=results,
        in_specs=[vmem] * 4,
        out_specs=[pl.BlockSpec(memory_space=pltpu.HBM)] * 4,
        scratch_shapes=[dma((4,))],
        compiler_params=pltpu.CompilerParams(vmem_limit_bytes=8 << 20),
    )(*made)
    return (
        flat.reshape(C, X, Y, Z),
        wflat.reshape(3, 3, 3, C, C).transpose(3, 4, 0, 1, 2),
        gain_grad.reshape(C),
        shift_grad.reshape(C),
    )


def solution(mesh):
    sizes = tuple(mesh.shape[name] for name in ("gx", "gy", "gz"))
    spec = P(None, "gx", "gy", "gz")
    return jax.shard_map(
        functools.partial(shards, sizes),
        mesh=mesh,
        in_specs=(spec, P(), P(), P(), spec),
        out_specs=(spec, P(), P(), P()),
        check_vma=False,
    )
```

```python
import functools

import jax
import jax.numpy as jnp
from jax import lax
from jax.experimental import pallas as pl
from jax.experimental.pallas import tpu as pltpu
from jax.sharding import PartitionSpec as P

MESH = pl.DeviceIdType.MESH
L = 128
C = 16
ROWS = 9 * C
BF = jnp.bfloat16
F32 = jnp.float32
SIDES = [(sx, sy) for sx in (-1, 0, 1) for sy in (-1, 0, 1) if (sx, sy) != (0, 0)]


def split(v):
    hi = v.astype(BF)
    lo = (v - hi.astype(F32)).astype(BF)
    return hi, lo


def kernel(
    dims, count, vol_ref, cot_ref, w_ref, gain_ref, shift_ref,
    out_ref, wout_ref, gout_ref, bout_ref,
    vin, cin, wv, gv, bv, mf_ref, mb_ref, ev, ec, eo, ea, hv, hc, ho, ha, cbv, cbc, cbo,
    r_ref, o_ref, agp, cvp, acc_ref, gw, gfull,
    z1, p1, z2, p2, gp_buf, gy_buf, gf_buf,
    in_sem, hsend, hrecv, asend, arecv, gsend, grecv,
):
    nx, ny, nz, X, Y = dims
    W = (Y + 2) * L
    I0, I1 = L, (Y + 1) * L
    mx, my, mz = lax.axis_index("gx"), lax.axis_index("gy"), lax.axis_index("gz")
    lane = lax.broadcasted_iota(jnp.int32, (C, L), 1)
    sub = lax.broadcasted_iota(jnp.int32, (C, L), 0)
    half = L // 2
    npl = nx * nz
    xs_at = [mx] + [lax.rem(mx + d, nx) for d in range(1, nx)]
    ys_at = [my] + [lax.rem(my + d, ny) for d in range(1, ny)]
    zs_at = [mz] + [lax.rem(mz + d, nz) for d in range(1, nz)]
    xs_row = [x * nz for x in xs_at]
    mp = xs_row[0] + mz
    plane = (
        mp, npl,
        [
            ({"gx": xs_at[dx], "gz": zs_at[dz]}, xs_row[dx] + zs_at[dz])
            for dx in range(nx)
            for dz in range(nz)
            if dx or dz
        ],
    )
    line = (my, ny, [({"gy": ys_at[d]}, ys_at[d]) for d in range(1, ny)])

    def side_id(sx, sy):
        out = {}
        if sx:
            out["gx"] = xs_at[sx]
        if sy:
            out["gy"] = ys_at[sy]
        return out

    loads = [
        pltpu.make_async_copy(src, dst, in_sem.at[k])
        for k, (src, dst) in enumerate(
            ((vol_ref, vin), (cot_ref, cin), (w_ref, wv), (gain_ref, gv), (shift_ref, bv))
        )
    ]
    for copy in loads:
        copy.start()

    barrier = pltpu.get_barrier_semaphore()
    greets = 0
    for group in (plane, line):
        for there, _ in group[2]:
            pl.semaphore_signal(barrier, inc=1, device_id=there, device_id_type=MESH)
            greets += 1
    for sx, sy in SIDES:
        if sx and sy:
            pl.semaphore_signal(barrier, inc=1, device_id=side_id(sx, sy), device_id_type=MESH)
            greets += 1

    def face(ref, sx, sy):
        src_x = {1: X, -1: 1, 0: pl.ds(1, X)}[sx]
        dst_x = {1: 0, -1: X + 1, 0: pl.ds(1, X)}[sx]
        src_y = {1: pl.ds(Y * L, L), -1: pl.ds(L, L), 0: pl.ds(I0, Y * L)}[sy]
        dst_y = {1: pl.ds(0, L), -1: pl.ds(I1, L), 0: pl.ds(I0, Y * L)}[sy]
        return ref.at[src_x, :, src_y], ref.at[dst_x, :, dst_y]

    def await_bytes(ref, sem):
        pltpu.make_async_copy(ref, ref, sem).wait()

    def face_copy(which, ref, k):
        sx, sy = SIDES[k]
        src, dst = face(ref, sx, sy)
        kind = 2 if sx and sy else (0 if sx else 1)
        return pltpu.make_async_remote_copy(
            src_ref=src, dst_ref=dst, send_sem=hsend.at[which, kind], recv_sem=hrecv.at[which, kind],
            device_id=side_id(sx, sy), device_id_type=MESH,
        )

    def col_copy(which, cb, k):
        s = 1 - 2 * k
        return pltpu.make_async_remote_copy(
            src_ref=cb.at[k], dst_ref=cb.at[2 + k],
            send_sem=hsend.at[which, 3], recv_sem=hrecv.at[which, 3],
            device_id={"gz": zs_at[s]}, device_id_type=MESH,
        )

    def tile_copy(which, h, k):
        sx, sy = SIDES[k]
        kind = 4 if sx else 5
        return pltpu.make_async_remote_copy(
            src_ref=h.at[4], dst_ref=h.at[(1 - sx) * 3 + (1 - sy)],
            send_sem=hsend.at[which, kind], recv_sem=hrecv.at[which, kind],
            device_id=side_id(sx, sy), device_id_type=MESH,
        )

    def send_cols(which, cb):
        for k in range(2):
            col_copy(which, cb, k).start()

    def send_faces(which, e):
        for k in (1, 6, 3, 4, 0, 2, 5, 7):
            face_copy(which, e, k).start()

    def pass_tiles(which, cb, h):
        await_bytes(cb.at[pl.ds(2, 2)], hrecv.at[which, 3])
        h[4] = jnp.where(lane < half, cb[2], cb[3])
        for k in range(8):
            tile_copy(which, h, k).start()

    def edges_done(e, h, sems):
        await_bytes(e.at[pl.ds(1, X), :, pl.ds(0, 2 * L)], sems.at[1])
        await_bytes(h.at[pl.ds(0, 2)], sems.at[5])

    def sides_done(e, h, sems):
        await_bytes(e.at[pl.ds(0, 2), :, pl.ds(I0, Y * L)], sems.at[0])
        await_bytes(e.at[0, :, pl.ds(0, 4 * L)], sems.at[2])
        await_bytes(h.at[pl.ds(0, 6)], sems.at[4])

    def wait_edges(which, e, h):
        edges_done(e, h, hrecv.at[which])

    def wait_sides(which, e, h):
        sides_done(e, h, hrecv.at[which])

    def wait_halo(which, e, h):
        wait_edges(which, e, h)
        wait_sides(which, e, h)

    def drain_halo(which, e, cb, h):
        edges_done(e, h, hsend.at[which])
        sides_done(e, h, hsend.at[which])
        await_bytes(cb.at[pl.ds(0, 2)], hsend.at[which, 3])

    def peer(buf, group, ss, rs, one):
        there, own = one[0], group[0]
        return pltpu.make_async_remote_copy(
            src_ref=buf.at[own], dst_ref=buf.at[own], send_sem=ss, recv_sem=rs,
            device_id=there, device_id_type=MESH,
        )

    def arrive(buf, group, ss, rs):
        await_bytes(buf.at[pl.ds(0, group[1] - 1)], rs)

    def start(spec, value):
        spec[0][spec[1][0]] = value
        for one in spec[1][2]:
            peer(*spec, one).start()

    def slots(buf, n):
        total = [buf[j] for j in range(n)]
        while len(total) > 1:
            total = [
                total[j] + total[j + 1] if j + 1 < len(total) else total[j]
                for j in range(0, len(total), 2)
            ]
        return total[0]

    def finish(spec):
        arrive(*spec)
        return slots(spec[0], spec[1][1])

    def settle(spec):
        await_bytes(spec[0].at[pl.ds(0, spec[1][1] - 1)], spec[2])

    s_z1 = (z1, line, asend.at[0], arecv.at[0])
    s_p1 = (p1, plane, asend.at[1], arecv.at[1])
    s_z2 = (z2, line, asend.at[2], arecv.at[2])
    s_p2 = (p2, plane, asend.at[3], arecv.at[3])
    g_y = (gy_buf, line, gsend.at[1], grecv.at[1])
    g_f = (gf_buf, plane, gsend.at[2], grecv.at[2])

    def pack(columns):
        tile = jnp.zeros((C, L), F32)
        for j, col in enumerate(columns):
            tile = jnp.where(lane == sub + j * C, col, tile)
        return jnp.sum(tile, axis=0, keepdims=True)

    def unpack(row, j):
        return jnp.sum(jnp.where(lane == sub + j * C, row, 0.0), axis=1, keepdims=True)

    def bring(src, e, cb):
        def body(x, cols):
            right, left = cols
            for y in range(Y):
                t = src[pl.ds(x * Y + y, C, stride=X * Y), :]
                e[x + 1, :, (y + 1) * L : (y + 2) * L] = t
                at = x * Y + y
                right = jnp.where(lane == at, pltpu.roll(t, at + 1, 1), right)
                left = jnp.where(lane == at + half, pltpu.roll(t, at + half, 1), left)
            return right, left

        zero = jnp.zeros((C, L), F32)
        right, left = lax.fori_loop(0, X, body, (zero, zero))
        cb[0] = right
        cb[1] = left

    def columns_of(e, cb):
        def body(x, cols):
            right, left = cols
            for y in range(Y):
                t = e[x + 1, :, (y + 1) * L : (y + 2) * L]
                at = x * Y + y
                right = jnp.where(lane == at, pltpu.roll(t, at + 1, 1), right)
                left = jnp.where(lane == at + half, pltpu.roll(t, at + half, 1), left)
            return right, left

        zero = jnp.zeros((C, L), F32)
        right, left = lax.fori_loop(0, X, body, (zero, zero))
        cb[0] = right
        cb[1] = left

    def build(e, h, xp, dx, xs, blocks):
        for yb in blocks:
            dy = -1 if yb == 0 else (1 if yb == Y + 1 else 0)
            ys = Y - 1 if yb == 0 else (0 if yb == Y + 1 else yb - 1)
            slot = (dx + 1) * 3 + dy + 1
            at = xs * Y + ys
            t = e[xp, :, yb * L : (yb + 1) * L]
            before = pltpu.roll(h[slot], lax.rem(L - at, L), 1)
            after = pltpu.roll(h[slot], half - 1 - at, 1)
            low = jnp.where(lane == 0, before, pltpu.roll(t, 1, 1))
            high = jnp.where(lane == L - 1, after, pltpu.roll(t, L - 1, 1))
            for c, v in enumerate((low, t, high)):
                hi, lo = split(v)
                r_ref[xp, c * C : (c + 1) * C, yb * L : (yb + 1) * L] = hi
                r_ref[xp, (3 + c) * C : (4 + c) * C, yb * L : (yb + 1) * L] = lo

    def taps(xp, lo, hi):
        r = r_ref[xp, :, lo:hi]
        return jnp.concatenate([r, r[0 : 3 * C]], axis=0)

    def spread(m_ref, xp, lo, hi, which):
        part = jnp.dot(
            m_ref[which[0] * 3 * C : (which[-1] + 1) * 3 * C, :], taps(xp, lo, hi),
            preferred_element_type=F32,
        )
        for ia, a in enumerate(which):
            for b in range(3):
                row = (ia * 3 + b) * C
                at = lo + (2 - b) * L
                o_ref[xp - a + 2, :, at : at + hi - lo] += part[row : row + C]

    def clear():
        def body(x, carry):
            o_ref[x] = jnp.zeros((C, (Y + 4) * L), F32)
            return carry

        lax.fori_loop(0, X + 4, body, 0)

    def interior(m_ref, e, h):
        def body(x, carry):
            build(e, h, x + 1, 0, x, range(1, Y + 1))
            spread(m_ref, x + 1, I0, I1, (0, 1, 2))
            return carry

        lax.fori_loop(0, X, body, 0)

    def edges(m_ref, e, h):
        def body(x, carry):
            build(e, h, x + 1, 0, x, (0, Y + 1))
            spread(m_ref, x + 1, 0, L, (0, 1, 2))
            spread(m_ref, x + 1, I1, I1 + L, (0, 1, 2))
            return carry

        lax.fori_loop(0, X, body, 0)

    def rim(m_ref, e, h):
        build(e, h, 0, -1, X - 1, range(Y + 2))
        spread(m_ref, 0, 0, W, (0,))
        build(e, h, X + 1, 1, 0, range(Y + 2))
        spread(m_ref, X + 1, 0, W, (2,))

    def clear_pad(ref):
        for x in range(X):
            ref[x, :, 0 : 2 * L] = jnp.zeros((2 * C, 2 * L), BF)
            ref[x, :, (Y + 2) * L : (Y + 4) * L] = jnp.zeros((2 * C, 2 * L), BF)

    def put_pad(ref, x, v):
        hi, lo = split(v)
        ref[x, 0:C, 2 * L : (Y + 2) * L] = hi
        ref[x, C : 2 * C, 2 * L : (Y + 2) * L] = lo

    def correlate(ref):
        acc_ref[...] = jnp.zeros((2 * ROWS, L), F32)
        for xp in range(X + 2):
            valid = [a for a in range(3) if 0 <= xp - a < X]
            left = jnp.concatenate(
                [
                    ref[xp - a, :, (2 - b) * L : (2 - b) * L + W]
                    for a in valid
                    for b in range(3)
                ],
                axis=0,
            )
            at = valid[0] * 6 * C
            acc_ref[at : at + left.shape[0], 0 : 6 * C] += lax.dot_general(
                left, r_ref[xp], (((1,), (1,)), ((), ())), preferred_element_type=F32
            )
        pieces = []
        for k in range(9):
            t = acc_ref[2 * k * C : (2 * k + 1) * C] + acc_ref[(2 * k + 1) * C : (2 * k + 2) * C]
            pieces.append(t + pltpu.roll(t, L - 3 * C, 1))
        return pieces

    def put_weights(m_ref, k, t):
        hi = t.astype(BF).astype(F32)
        m_ref[k * C : (k + 1) * C, :] = jnp.concatenate([hi, hi, t - hi], axis=1).astype(BF)

    def weights_forward():
        for k in range(9):
            at = k * 3 * C
            put_weights(
                mf_ref, k,
                jnp.concatenate([wv[at + c * C : at + (c + 1) * C] for c in range(3)], axis=1),
            )

    def weights_backward():
        for k in range(9):
            at = (8 - k) * 3 * C
            put_weights(
                mb_ref, k,
                jnp.concatenate(
                    [wv[at + c * C : at + (c + 1) * C] for c in (2, 1, 0)], axis=0
                ).T,
            )

    def as_column(ref):
        square = lax.broadcasted_iota(jnp.int32, (C, C), 0) == lax.broadcasted_iota(
            jnp.int32, (C, C), 1
        )
        return jnp.sum(jnp.where(square, ref[...], 0.0), axis=1, keepdims=True)

    loads[0].wait()
    bring(vin, ev, cbv)
    pl.semaphore_wait(barrier, greets)
    send_cols(0, cbv)
    send_faces(0, ev)
    for copy in loads[1:]:
        copy.wait()
    clear()
    weights_forward()
    bring(cin, ec, cbc)
    pass_tiles(0, cbv, hv)
    send_cols(1, cbc)
    interior(mf_ref, ev, hv)
    clear_pad(agp)
    clear_pad(cvp)
    weights_backward()

    def vol_sum(x, s):
        return s + jnp.sum(ev[x + 1, :, I0:I1], axis=1, keepdims=True)

    in_sum = lax.fori_loop(0, X, vol_sum, jnp.zeros((C, 1), F32))
    wait_edges(0, ev, hv)
    edges(mf_ref, ev, hv)
    wait_sides(0, ev, hv)
    send_faces(1, ec)
    rim(mf_ref, ev, hv)

    def gather_conv(x, sums):
        s, q = sums
        t = o_ref[x + 2, :, 2 * L : (Y + 2) * L]
        eo[x + 1, :, I0:I1] = t
        return (
            s + jnp.sum(t, axis=1, keepdims=True),
            q + jnp.sum(t * t, axis=1, keepdims=True),
        )

    zero_col = jnp.zeros((C, 1), F32)
    s, q = lax.fori_loop(0, X, gather_conv, (zero_col, zero_col))
    start(s_z1, pack((s, q, in_sum)))
    columns_of(eo, cbo)
    send_cols(2, cbo)

    def pad_conv(x, carry):
        put_pad(cvp, x, eo[x + 1, :, I0:I1])
        return carry

    lax.fori_loop(0, X, pad_conv, 0)
    part = finish(s_z1)
    start(s_p1, part)
    send_faces(2, eo)
    pass_tiles(1, cbc, hc)
    cross = correlate(cvp)
    for k in range(9):
        gw[k * C : (k + 1) * C] = pltpu.roll(cross[k], half, 1)
    pass_tiles(2, cbo, ho)
    clear()
    gain = as_column(gv)
    shift = as_column(bv)
    total1 = finish(s_p1)
    mean = unpack(total1, 0) / count
    var = unpack(total1, 1) / count - mean * mean
    rstd = lax.rsqrt(var + 1e-05)

    def slope(conv, cot):
        normed = (conv - mean) * rstd
        act = gain * normed + shift
        sig = 1.0 / (1.0 + jnp.exp(-act))
        return cot * sig * (1.0 + act * (1.0 - sig)), normed

    def local_slope(x, sums):
        sg, sb = sums
        a, normed = slope(eo[x + 1, :, I0:I1], ec[x + 1, :, I0:I1])
        ea[x + 1, :, I0:I1] = a
        put_pad(agp, x, a)
        return (
            sg + jnp.sum(a * normed, axis=1, keepdims=True),
            sb + jnp.sum(a, axis=1, keepdims=True),
        )

    sg, sb = lax.fori_loop(0, X, local_slope, (zero_col, zero_col))
    start(s_z2, pack((sg, sb)))
    cross = correlate(agp)
    for k in range(9):
        gw[k * C : (k + 1) * C] = jnp.where(lane < half, cross[k], gw[k * C : (k + 1) * C])
    if gw.shape[0] > ROWS:
        gw[ROWS:] = jnp.zeros((gw.shape[0] - ROWS, L), F32)
    chunk = gw.shape[0] // npl

    def piece(j):
        return gw.at[pl.ds(pl.multiple_of(j * chunk, 8), chunk)]

    def scatter(one):
        there, to = one
        return pltpu.make_async_remote_copy(
            src_ref=piece(to), dst_ref=gp_buf.at[mp], send_sem=gsend.at[0], recv_sem=grecv.at[0],
            device_id=there, device_id_type=MESH,
        )

    gp_buf[mp] = gw[pl.ds(pl.multiple_of(mp * chunk, 8), chunk)]
    for one in plane[2]:
        scatter(one).start()

    part = finish(s_z2)
    start(s_p2, part)
    await_bytes(gp_buf.at[pl.ds(0, npl - 1)], grecv.at[0])
    start(g_y, slots(gp_buf, npl))
    wait_halo(1, ec, hc)
    wait_halo(2, eo, ho)
    for xp in (0, X + 1):
        a, _ = slope(eo[xp], ec[xp])
        ea[xp] = a

    def edge_slope(x, carry):
        for at in (0, I1):
            a, _ = slope(eo[x + 1, :, at : at + L], ec[x + 1, :, at : at + L])
            ea[x + 1, :, at : at + L] = a
        return carry

    lax.fori_loop(0, X, edge_slope, 0)

    def tile_slope(k, carry):
        a, _ = slope(ho[k], hc[k])
        ha[k] = a
        return carry

    lax.fori_loop(0, 9, tile_slope, 0)

    total2 = finish(s_p2)
    gain_grad = unpack(total2, 0)
    shift_grad = unpack(total2, 1)
    scale = gain * rstd
    k_conv = -scale * rstd * (gain_grad / count)
    k_one = -scale * (shift_grad / count) - k_conv * mean

    def blend(xp, carry):
        ea[xp] = scale * ea[xp] + k_conv * eo[xp] + k_one
        return carry

    lax.fori_loop(0, X + 2, blend, 0)

    def blend_tile(k, carry):
        ha[k] = scale * ha[k] + k_conv * ho[k] + k_one
        return carry

    lax.fori_loop(0, 9, blend_tile, 0)
    gpart = finish(g_y)
    start(g_f, gpart)
    interior(mb_ref, ea, ha)
    edges(mb_ref, ea, ha)
    rim(mb_ref, ea, ha)

    def emit(x, carry):
        for y in range(Y):
            out_ref[pl.ds(x * Y + y, C, stride=X * Y), :] = o_ref[
                x + 2, :, (y + 2) * L : (y + 3) * L
            ]
        return carry

    lax.fori_loop(0, X, emit, 0)
    gout_ref[...] = total2[:, 0:C]
    bout_ref[...] = pltpu.roll(total2, L - C, 1)[:, 0:C]
    wide = jnp.sum(
        jnp.where(lax.rem(lane, C) == sub, unpack(total1, 2), 0.0), axis=0, keepdims=True
    )
    k_norm = scale * rstd * (gain_grad / count)
    k_wide = (k_norm * mean - scale * (shift_grad / count)) * wide
    drain_halo(0, ev, cbv, hv)
    drain_halo(1, ec, cbc, hc)
    drain_halo(2, eo, cbo, ho)
    for spec in (s_z1, s_p1, s_z2, s_p2, g_y):
        settle(spec)
    await_bytes(gp_buf.at[pl.ds(0, npl - 1)], gsend.at[0])
    arrive(*g_f)
    if chunk != 8:
        for j in range(npl):
            gfull[j * chunk : (j + 1) * chunk] = gf_buf[j]
    for k in range(9):
        if chunk == 8:
            t = jnp.concatenate([gf_buf[2 * k], gf_buf[2 * k + 1]], axis=0)
        else:
            t = gfull[k * C : (k + 1) * C]
        t = scale * t - k_norm * pltpu.roll(t, half, 1) + k_wide
        for c in range(3):
            at = (k * 3 + c) * C
            wout_ref[at : at + C, :] = (t if c == 0 else pltpu.roll(t, L - c * C, 1))[:, 0:C]
    settle(g_f)


def store(*refs):
    n = len(refs) // 2
    sem = refs[-1]
    copies = [
        pltpu.make_async_copy(refs[k], refs[n + k], sem.at[k]) for k in range(n)
    ]
    for copy in copies:
        copy.start()
    for copy in copies:
        copy.wait()


def shards(sizes, volume, weight, gamma, beta, cotangent):
    nx, ny, nz = sizes
    _, X, Y, Z = volume.shape
    count = float(X * Y * Z * nx * ny * nz)
    W = (Y + 2) * L
    npl = nx * nz
    chunk = -(-(ROWS // 8) // npl) * 8
    rows = chunk * npl
    vmem = pl.BlockSpec(memory_space=pltpu.VMEM)
    e_shape = pltpu.VMEM((X + 2, C, W), F32)
    h_shape = pltpu.VMEM((9, C, L), F32)
    cb_shape = pltpu.VMEM((4, C, L), F32)
    pad_shape = pltpu.VMEM((X, 2 * C, (Y + 4) * L), BF)
    m_shape = pltpu.VMEM((ROWS, ROWS), BF)
    line_rows = pltpu.VMEM((ny, 1, L), F32)
    plane_rows = pltpu.VMEM((npl, 1, L), F32)
    dma = pltpu.SemaphoreType.DMA
    results = (
        jax.ShapeDtypeStruct((C * X * Y, L), F32),
        jax.ShapeDtypeStruct((27 * C, C), F32),
        jax.ShapeDtypeStruct((1, C), F32),
        jax.ShapeDtypeStruct((1, C), F32),
    )
    made = pl.pallas_call(
        functools.partial(kernel, (nx, ny, nz, X, Y), count),
        out_shape=results,
        in_specs=[pl.BlockSpec(memory_space=pltpu.HBM)] * 5,
        out_specs=(vmem, vmem, vmem, vmem),
        scratch_shapes=[
            pltpu.VMEM((C * X * Y, L), F32), pltpu.VMEM((C * X * Y, L), F32),
            pltpu.VMEM((27 * C, C), F32), pltpu.VMEM((1, C), F32), pltpu.VMEM((1, C), F32),
            m_shape, m_shape,
            e_shape, e_shape, e_shape, e_shape,
            h_shape, h_shape, h_shape, h_shape,
            cb_shape, cb_shape, cb_shape,
            pltpu.VMEM((X + 2, 6 * C, W), BF),
            pltpu.VMEM((X + 4, C, (Y + 4) * L), F32),
            pad_shape, pad_shape,
            pltpu.VMEM((2 * ROWS, L), F32),
            pltpu.VMEM((rows, L), F32), pltpu.VMEM((rows, L), F32),
            line_rows, plane_rows, line_rows, plane_rows,
            pltpu.VMEM((npl, chunk, L), F32), pltpu.VMEM((ny, chunk, L), F32),
            pltpu.VMEM((npl, chunk, L), F32),
            dma((5,)), dma((3, 6)), dma((3, 6)), dma((4,)), dma((4,)), dma((3,)), dma((3,)),
        ],
        compiler_params=pltpu.CompilerParams(
            collective_id=0, has_side_effects=True, vmem_limit_bytes=24 << 20
        ),
    )(
        *(
            pltpu.with_memory_space_constraint(v, pltpu.HBM)
            for v in (
                volume.reshape(C * X * Y, L), cotangent.reshape(C * X * Y, L),
                weight.transpose(2, 3, 4, 0, 1).reshape(27 * C, C),
                gamma.reshape(1, C), beta.reshape(1, C),
            )
        )
    )
    flat, wflat, gain_grad, shift_grad = pl.pallas_call(
        store,
        out_shape=results,
        in_specs=[vmem] * 4,
        out_specs=[pl.BlockSpec(memory_space=pltpu.HBM)] * 4,
        scratch_shapes=[dma((4,))],
        compiler_params=pltpu.CompilerParams(vmem_limit_bytes=8 << 20),
    )(*made)
    return (
        flat.reshape(C, X, Y, Z),
        wflat.reshape(3, 3, 3, C, C).transpose(3, 4, 0, 1, 2),
        gain_grad.reshape(C),
        shift_grad.reshape(C),
    )


def solution(mesh):
    sizes = tuple(mesh.shape[name] for name in ("gx", "gy", "gz"))
    spec = P(None, "gx", "gy", "gz")
    return jax.shard_map(
        functools.partial(shards, sizes),
        mesh=mesh,
        in_specs=(spec, P(), P(), P(), spec),
        out_specs=(spec, P(), P(), P()),
        check_vma=False,
    )
```
